32 devices in a mesh: outer: 8 (over z, x), inner: 4 (over y, core).
Axes of the slice: x: 2, y: 2, z: 4, core: 2. Of those that a mesh axis runs over, the one named last changes fastest.
Arguments:
- queries: bfloat16 [1024, 2, 4096], P('outer', None, 'inner'), may hold values from -52 to 52
- keys: bfloat16 [1024, 2, 4096], P('outer', None, 'inner'), may hold values from -6 to 6
- values: bfloat16 [1024, 2, 4096], P('outer', None, 'inner'), may hold values from -6 to 6
Outputs:
- attended: bfloat16 [1024, 2, 4096], P(('outer', 'inner'))
The draws below stay inside these ranges and needn't reach their ends.
All inputs are finite; a program needn't handle non-finite values.
Results may differ from the reference program's by a relative error of at most 0.004.
Values may be sent and summed in bfloat16 or wider, within the bound.
A program may use at most 128 MiB of HBM per device.

```python
import math
import jax
import jax.numpy as jnp
from jax import lax

NETWORKS = 2
HEADS = 32
HEAD_DIM = 128
WIDTH = 4096
SEQ = 1024


def key_field(key):
    base = jax.random.fold_in(key, 11)
    field = jnp.clip(jax.random.normal(base, (SEQ, NETWORKS, WIDTH), jnp.float32), -6.0, 6.0)
    return field


def draw_keys(key, part):
    return key_field(key).astype(jnp.bfloat16)


def draw_queries(key, part):
    base = jax.random.fold_in(key, 12)
    result = 3.0 * jnp.clip(jax.random.normal(base, (SEQ, NETWORKS, WIDTH), jnp.float32), -6.0, 6.0)
    return result.astype(jnp.bfloat16)


def steps_of(rng, shape, shards, low, high):
    factor_of, own = 1.0, jax.random.fold_in(rng, 6)
    for axis_at, shards_of in shards:
        draws = jnp.exp(jax.random.uniform(jax.random.fold_in(own, axis_at), (shards_of,), jnp.float32, low / len(shards), high / len(shards)))
        factor_of = factor_of * jnp.repeat(draws, shape[axis_at] // shards_of).reshape([-1 if axis == axis_at else 1 for axis in range(len(shape))])
    return factor_of


def scatter_about(rng, extent, scale, reach, pieces=(), kind=jnp.bfloat16):
    gain = steps_of(rng, extent, pieces, -0.22, 0.18) if pieces else 1.0
    values = jax.random.normal(rng, extent, jnp.float32) * scale * gain
    return jnp.minimum(jnp.maximum(values, -reach), reach).astype(kind)


def setup_inputs(seed: int = 0) -> dict:
    splits = jax.random.split(jax.random.key(seed), 4)
    queries = draw_queries(jax.random.fold_in(splits[3], 71), 0)
    keys = draw_keys(jax.random.fold_in(splits[3], 71), 0)
    values = scatter_about(splits[2], (SEQ, NETWORKS, WIDTH), 1.0, 6.0, ((0, 8), (2, 4)))
    return dict(queries=queries, keys=keys, values=values)


def attend_rows(query_rows, key_rows, value_rows):
    scores = jnp.dot(query_rows, key_rows.T, preferred_element_type=jnp.float32) * (1.0 / math.sqrt(HEAD_DIM))
    peak_rows = lax.optimization_barrier(jnp.max(scores, axis=1, keepdims=True))
    weights = jnp.exp(scores - peak_rows)
    totals = lax.optimization_barrier(jnp.sum(weights, axis=1, keepdims=True))
    numerator = jnp.dot(weights.astype(jnp.bfloat16), value_rows, preferred_element_type=jnp.float32)
    return numerator / totals

def attend_pair(inputs):
    query_rows, key_rows, value_rows = inputs
    blocks = query_rows.reshape(16, SEQ // 16, HEAD_DIM)
    result = lax.map(lambda block: attend_rows(block, key_rows, value_rows), blocks)
    return result.reshape(SEQ, HEAD_DIM)

def split_heads(array):
    return array.reshape(SEQ, NETWORKS, HEADS, HEAD_DIM).transpose(1, 2, 0, 3).reshape(NETWORKS * HEADS, SEQ, HEAD_DIM)

def reference(queries, keys, values):
    averaged = lax.map(attend_pair, (split_heads(queries), split_heads(keys), split_heads(values)))
    averaged = averaged.reshape(NETWORKS, HEADS, SEQ, HEAD_DIM).transpose(2, 0, 1, 3)
    return averaged.reshape(SEQ, NETWORKS, WIDTH).astype(jnp.bfloat16)
```

```python
from functools import partial
import math

import jax
import jax.numpy as jnp
from jax import lax
from jax.experimental import pallas as pl
from jax.experimental.pallas import tpu as pltpu
from jax.sharding import PartitionSpec as P

HEAD_DIM = 128
MESH = pl.DeviceIdType.MESH


def attend_keys(running, key_block, value_block, query_heads, head_count):
    peak_rows, totals, numerator = running
    key_count = key_block.shape[0]
    key_heads = key_block.reshape(key_count, head_count, HEAD_DIM)
    value_heads = value_block.reshape(key_count, head_count, HEAD_DIM)
    scores = jnp.einsum(
        "qhd,khd->qhk", query_heads, key_heads, preferred_element_type=jnp.float32
    ) * (1.0 / math.sqrt(HEAD_DIM))
    new_peaks = jnp.maximum(peak_rows, jnp.max(scores, axis=2))
    shrink = jnp.exp(peak_rows - new_peaks)
    weights = jnp.exp(scores - new_peaks[..., None])
    totals = totals * shrink + jnp.sum(weights, axis=2)
    numerator = numerator * shrink[..., None] + jnp.einsum(
        "qhk,khd->qhd",
        weights.astype(jnp.bfloat16),
        value_heads,
        preferred_element_type=jnp.float32,
    )
    return (new_peaks, totals, numerator)


def attend_piece(running, pieces, query_part, head_count):
    key_rows, value_rows = pieces
    row_count = query_part.shape[0]
    query_heads = query_part.reshape(row_count, head_count, HEAD_DIM)
    block_count = key_rows.shape[0] // row_count
    key_blocks = key_rows.reshape(block_count, row_count, key_rows.shape[1])
    value_blocks = value_rows.reshape(block_count, row_count, value_rows.shape[1])

    def one_block(state, blocks):
        return (attend_keys(state, blocks[0], blocks[1], query_heads, head_count), None)

    running, unused = lax.scan(one_block, running, (key_blocks, value_blocks))
    return running


def start_state(row_count, head_count):
    peak_rows = jnp.full((row_count, head_count), -jnp.inf, jnp.float32)
    totals = jnp.zeros((row_count, head_count), jnp.float32)
    numerator = jnp.zeros((row_count, head_count, HEAD_DIM), jnp.float32)
    return (peak_rows, totals, numerator)


def finish_state(running):
    peak_rows, totals, numerator = running
    averaged = numerator / totals[..., None]
    return averaged.reshape(numerator.shape[0], -1).astype(jnp.bfloat16)


def flatten(array):
    return array.reshape(array.shape[0], array.shape[1] * array.shape[2])


def per_device_split(queries, keys, values):
    tok_rows, networks, local_cols = queries.shape
    full_q, full_k, full_v = (
        lax.all_to_all(array, "inner", split_axis=0, concat_axis=2, tiled=True)
        for array in (queries, keys, values)
    )
    unit_rows = full_q.shape[0]
    full_cols = full_q.shape[2]
    query_part, key_part, value_part = (
        lax.all_to_all(flatten(array), "outer", split_axis=1, concat_axis=0, tiled=True)
        for array in (full_q, full_k, full_v)
    )
    head_count = query_part.shape[1] // HEAD_DIM
    running = attend_piece(
        start_state(query_part.shape[0], head_count),
        (
            lax.all_gather(key_part, "inner", axis=0, tiled=True),
            lax.all_gather(value_part, "inner", axis=0, tiled=True),
        ),
        query_part,
        head_count,
    )
    gathered = lax.all_to_all(
        finish_state(running), "outer", split_axis=0, concat_axis=1, tiled=True
    )
    return gathered.reshape(unit_rows, networks, full_cols)


def attend_block(query, key, value):
    raw = lax.dot_general(
        query, key, (((1,), (1,)), ((), ())), preferred_element_type=jnp.float32
    )
    peak = jnp.max(raw, axis=1, keepdims=True)
    weights = jnp.exp2((raw - peak) * (math.log2(math.e) / math.sqrt(HEAD_DIM)))
    totals = jnp.sum(weights, axis=1, keepdims=True)
    numerator = jnp.dot(
        weights.astype(jnp.bfloat16), value, preferred_element_type=jnp.float32
    )
    return (numerator / totals).astype(jnp.bfloat16)


COLUMNS = 2


def exchange_kernel(
    outer, inner, heads,
    q_ref, k_ref, v_ref, out_ref,
    q_raw, k_raw, v_raw, k_buf, v_buf, o_raw,
    q_src, k_src, v_src, src_sem, local_sem, in_send, in_recv, out_send, out_recv, ready,
):
    me_o, me_i = lax.axis_index("outer"), lax.axis_index("inner")
    tokens, networks, local_cols = q_ref.shape
    out_rows = out_ref.shape[0]
    rows, half = outer // COLUMNS, outer // COLUMNS // 2
    row, col = me_o // COLUMNS, me_o % COLUMNS
    near_side = half * COLUMNS - 1
    refs, raws = (k_src, v_src, q_src), (k_raw, v_raw, q_raw)

    def peer(slot, row, col, where):
        side = row // half
        turn = slot + 1
        same = side * half + (row + turn // COLUMNS) % half
        away = (slot - near_side) // COLUMNS
        other = where(side == 0, half + away, half - 1 - away)
        is_near = slot < near_side
        shift = where(is_near, turn, slot - near_side)
        return where(is_near, same, other), (col + shift) % COLUMNS

    def pick(test, yes, no):
        return yes if test else no

    def distances(slot):
        found = set()
        for r in range(rows):
            for c in range(COLUMNS):
                pr, pc = peer(slot, r, c, pick)
                found.add(abs(pr - r) + abs(pc - c))
        return sorted(found)

    def traced_peer(slot):
        pr, pc = peer(slot, row, col, jnp.where)
        return pr * COLUMNS + pc, jnp.abs(pr - row) + jnp.abs(pc - col)

    def rows_of(block):
        return pl.ds(pl.multiple_of(block * tokens, tokens), tokens)

    def cols_of(head):
        return pl.ds(pl.multiple_of(head * HEAD_DIM, HEAD_DIM), HEAD_DIM)

    def in_copy(head, which, target, source, other):
        return pltpu.make_async_remote_copy(
            src_ref=refs[which].at[:, :, cols_of(target * heads + head)],
            dst_ref=raws[which].at[head, rows_of(source)],
            send_sem=in_send,
            recv_sem=in_recv.at[head * 3 + which, source],
            device_id=(other, me_i),
            device_id_type=MESH,
        )

    def send_in(head, which, other):
        in_copy(head, which, other, me_o, other).start()

    def wait_in(head, which, source):
        in_copy(head, which, me_o, source, source).wait_recv()

    def own_copy(head, which):
        return pltpu.make_async_copy(
            refs[which].at[:, :, cols_of(me_o * heads + head)],
            raws[which].at[head, rows_of(me_o)],
            local_sem.at[head * 3 + which],
        )

    def out_cols(source_o, source_i, head):
        return cols_of(source_i * (local_cols // HEAD_DIM) + source_o * heads + head)

    def out_slice(block, part):
        return pl.ds(block * tokens + part * out_rows, out_rows)

    def out_copy(head, block, part):
        return pltpu.make_async_remote_copy(
            src_ref=o_raw.at[head, out_slice(block, part)],
            dst_ref=out_ref.at[:, :, out_cols(me_o, me_i, head)],
            send_sem=out_send,
            recv_sem=out_recv,
            device_id=(block, part),
            device_id_type=MESH,
        )

    def out_own(head):
        return pltpu.make_async_copy(
            o_raw.at[head, out_slice(me_o, me_i)],
            out_ref.at[:, :, out_cols(me_o, me_i, head)],
            out_recv,
        )

    def tell(sem, device):
        pl.semaphore_signal(sem, inc=1, device_id=device, device_id_type=MESH)

    beside = [
        (row > 0, me_o - COLUMNS),
        (row < rows - 1, me_o + COLUMNS),
        (col > 0, me_o - 1),
        (col < COLUMNS - 1, me_o + 1),
    ]
    beside_count = sum(jnp.where(exists, 1, 0) for exists, other in beside)

    def tell_beside(sem):
        for exists, other in beside:
            @pl.when(exists)
            def _():
                tell(sem, (other, me_i))

    def meet(round_at):
        tell_beside(ready.at[round_at])
        pl.semaphore_wait(ready.at[round_at], beside_count)

    barrier = pltpu.get_barrier_semaphore()
    tell_beside(barrier)
    for shift in range(1, inner):
        tell(barrier, (me_o, (me_i + shift) % inner))
    sources = [
        pltpu.make_async_copy(ref, kept, src_sem.at[which])
        for which, (ref, kept) in enumerate(zip((k_ref, v_ref, q_ref), refs))
    ]
    for copy in sources:
        copy.start()
    for copy in sources[:2]:
        copy.wait()
    pl.semaphore_wait(barrier, beside_count + inner - 1)

    slots = [*range(near_side, outer - 1), *range(near_side)]
    furthest = rows + COLUMNS - 2
    for reach in range(1, furthest + 1):
        if reach > 1:
            meet(reach - 2)
        for slot in slots:
            lengths = distances(slot)
            if reach not in lengths:
                continue
            other, length = traced_peer(slot)

            def send_pair():
                for which in range(2):
                    send_in(0, which, other)

            if len(lengths) == 1:
                send_pair()
            else:
                pl.when(length == reach)(send_pair)
    sources[2].wait()
    for head in range(heads):
        for which in range(3):
            if head or which == 2:
                for slot in range(outer - 1):
                    send_in(head, which, traced_peer(slot)[0])
            own_copy(head, which).start()
    meet(furthest - 1)

    both = networks * tokens
    split_row = lax.broadcasted_iota(jnp.int32, (both, both), 0)
    split_col = lax.broadcasted_iota(jnp.int32, (both, both), 1)
    split = (split_col == (split_row % tokens) * networks + split_row // tokens)
    split = split.astype(jnp.float32).astype(jnp.bfloat16)
    join = (split_row == (split_col % tokens) * networks + split_col // tokens)
    join = join.astype(jnp.float32).astype(jnp.bfloat16)

    def separate(raw, head, block):
        mixed = raw[head, rows_of(block)].reshape(both, HEAD_DIM)
        return jnp.dot(split, mixed, preferred_element_type=jnp.float32).astype(jnp.bfloat16)

    def place(head, which, block):
        apart = separate(raws[which], head, block)
        kept = (k_buf, v_buf)[which]
        for network in range(networks):
            kept[network, rows_of(block)] = apart[network * tokens:(network + 1) * tokens]

    def compute(head, block):
        query = separate(q_raw, head, block)
        parts = [
            attend_block(query[n * tokens:(n + 1) * tokens], k_buf[n], v_buf[n])
            for n in range(networks)
        ]
        mixed = jnp.dot(join, jnp.concatenate(parts, axis=0), preferred_element_type=jnp.float32)
        o_raw[head, rows_of(block)] = mixed.astype(jnp.bfloat16).reshape(
            tokens, networks, HEAD_DIM
        )

    for head in range(heads):
        for which in range(3):
            own_copy(head, which).wait()
        for which in range(2):
            place(head, which, me_o)

        def one_place(slot, carry):
            block = traced_peer(slot)[0]
            for which in range(2):
                wait_in(head, which, block)
                place(head, which, block)
            return carry

        lax.fori_loop(0, outer - 1, one_place, 0)

        compute(head, me_o)
        for shift in range(1, inner):
            out_copy(head, me_o, (me_i + shift) % inner).start()
        out_own(head).start()

        def one_block(slot, carry):
            block = traced_peer(slot)[0]
            wait_in(head, 2, block)
            compute(head, block)
            for part in range(inner):
                out_copy(head, block, part).start()
            return carry

        lax.fori_loop(0, outer - 1, one_block, 0)

    def wait_bytes(ref, sem):
        pltpu.make_async_copy(ref, ref, sem).wait()

    for head in range(heads):
        for raw in raws:
            wait_bytes(raw.at[head, pl.ds(0, tokens * (outer - 1))], in_send)
        wait_bytes(o_raw.at[head, pl.ds(0, tokens * outer - out_rows)], out_send)
    wait_bytes(out_ref, out_recv)


def per_device(outer, inner, queries, keys, values):
    tokens, networks, local_cols = queries.shape
    heads = local_cols // HEAD_DIM // outer
    seq = tokens * outer
    out_rows = tokens // inner
    raw = pltpu.VMEM((heads, seq, networks, HEAD_DIM), jnp.bfloat16)
    kept = pltpu.VMEM((networks, seq, HEAD_DIM), jnp.bfloat16)
    return pl.pallas_call(
        partial(exchange_kernel, outer, inner, heads),
        out_shape=jax.ShapeDtypeStruct((out_rows, networks, local_cols * inner), jnp.bfloat16),
        in_specs=[pl.BlockSpec(memory_space=pl.ANY)] * 3,
        out_specs=pl.BlockSpec(memory_space=pl.ANY),
        scratch_shapes=[
            raw, raw, raw, kept, kept, raw,
            *[pltpu.VMEM(queries.shape, jnp.bfloat16)] * 3,
            pltpu.SemaphoreType.DMA((3,)),
            pltpu.SemaphoreType.DMA((heads * 3,)),
            pltpu.SemaphoreType.DMA,
            pltpu.SemaphoreType.DMA((heads * 3, outer)),
            pltpu.SemaphoreType.DMA,
            pltpu.SemaphoreType.DMA,
            pltpu.SemaphoreType.REGULAR((outer // COLUMNS + COLUMNS - 2,)),
        ],
        compiler_params=pltpu.CompilerParams(collective_id=0, has_side_effects=True, vmem_limit_bytes=54500 * 1024),
    )(queries, keys, values)


def solution(mesh):
    outer, inner = mesh.shape["outer"], mesh.shape["inner"]

    def body(queries, keys, values):
        heads = queries.shape[2] // HEAD_DIM
        if outer % (2 * COLUMNS) == 0 and heads % outer == 0:
            return per_device(outer, inner, queries, keys, values)
        return per_device_split(queries, keys, values)

    return jax.shard_map(
        body,
        mesh=mesh,
        in_specs=(P("outer", None, "inner"),) * 3,
        out_specs=P(("outer", "inner"), None, None),
        check_vma=False,
    )
```

```python
from functools import partial
import math

import jax
import jax.numpy as jnp
from jax import lax
from jax.experimental import pallas as pl
from jax.experimental.pallas import tpu as pltpu
from jax.sharding import PartitionSpec as P

HEAD_DIM = 128
MESH = pl.DeviceIdType.MESH


def attend_keys(running, key_block, value_block, query_heads, head_count):
    peak_rows, totals, numerator = running
    key_count = key_block.shape[0]
    key_heads = key_block.reshape(key_count, head_count, HEAD_DIM)
    value_heads = value_block.reshape(key_count, head_count, HEAD_DIM)
    scores = jnp.einsum(
        "qhd,khd->qhk", query_heads, key_heads, preferred_element_type=jnp.float32
    ) * (1.0 / math.sqrt(HEAD_DIM))
    new_peaks = jnp.maximum(peak_rows, jnp.max(scores, axis=2))
    shrink = jnp.exp(peak_rows - new_peaks)
    weights = jnp.exp(scores - new_peaks[..., None])
    totals = totals * shrink + jnp.sum(weights, axis=2)
    numerator = numerator * shrink[..., None] + jnp.einsum(
        "qhk,khd->qhd",
        weights.astype(jnp.bfloat16),
        value_heads,
        preferred_element_type=jnp.float32,
    )
    return (new_peaks, totals, numerator)


def attend_piece(running, pieces, query_part, head_count):
    key_rows, value_rows = pieces
    row_count = query_part.shape[0]
    query_heads = query_part.reshape(row_count, head_count, HEAD_DIM)
    block_count = key_rows.shape[0] // row_count
    key_blocks = key_rows.reshape(block_count, row_count, key_rows.shape[1])
    value_blocks = value_rows.reshape(block_count, row_count, value_rows.shape[1])

    def one_block(state, blocks):
        return (attend_keys(state, blocks[0], blocks[1], query_heads, head_count), None)

    running, unused = lax.scan(one_block, running, (key_blocks, value_blocks))
    return running


def start_state(row_count, head_count):
    peak_rows = jnp.full((row_count, head_count), -jnp.inf, jnp.float32)
    totals = jnp.zeros((row_count, head_count), jnp.float32)
    numerator = jnp.zeros((row_count, head_count, HEAD_DIM), jnp.float32)
    return (peak_rows, totals, numerator)


def finish_state(running):
    peak_rows, totals, numerator = running
    averaged = numerator / totals[..., None]
    return averaged.reshape(numerator.shape[0], -1).astype(jnp.bfloat16)


def flatten(array):
    return array.reshape(array.shape[0], array.shape[1] * array.shape[2])


def per_device_split(queries, keys, values):
    tok_rows, networks, local_cols = queries.shape
    full_q, full_k, full_v = (
        lax.all_to_all(array, "inner", split_axis=0, concat_axis=2, tiled=True)
        for array in (queries, keys, values)
    )
    unit_rows = full_q.shape[0]
    full_cols = full_q.shape[2]
    query_part, key_part, value_part = (
        lax.all_to_all(flatten(array), "outer", split_axis=1, concat_axis=0, tiled=True)
        for array in (full_q, full_k, full_v)
    )
    head_count = query_part.shape[1] // HEAD_DIM
    running = attend_piece(
        start_state(query_part.shape[0], head_count),
        (
            lax.all_gather(key_part, "inner", axis=0, tiled=True),
            lax.all_gather(value_part, "inner", axis=0, tiled=True),
        ),
        query_part,
        head_count,
    )
    gathered = lax.all_to_all(
        finish_state(running), "outer", split_axis=0, concat_axis=1, tiled=True
    )
    return gathered.reshape(unit_rows, networks, full_cols)


def attend_block(query, key, value):
    raw = lax.dot_general(
        query, key, (((1,), (1,)), ((), ())), preferred_element_type=jnp.float32
    )
    peak = jnp.max(raw, axis=1, keepdims=True)
    weights = jnp.exp2((raw - peak) * (math.log2(math.e) / math.sqrt(HEAD_DIM)))
    totals = jnp.sum(weights, axis=1, keepdims=True)
    numerator = jnp.dot(
        weights.astype(jnp.bfloat16), value, preferred_element_type=jnp.float32
    )
    return (numerator / totals).astype(jnp.bfloat16)


COLUMNS = 2


def exchange_kernel(
    outer, inner, heads,
    q_ref, k_ref, v_ref, out_ref,
    q_raw, k_raw, v_raw, k_buf, v_buf, o_raw,
    q_src, k_src, v_src, src_sem, local_sem, in_send, in_recv, out_send, out_recv, ready,
):
    me_o, me_i = lax.axis_index("outer"), lax.axis_index("inner")
    tokens, networks, local_cols = q_ref.shape
    out_rows = out_ref.shape[0]
    rows, half = outer // COLUMNS, outer // COLUMNS // 2
    row, col = me_o // COLUMNS, me_o % COLUMNS
    near_side = half * COLUMNS - 1
    refs, raws = (k_src, v_src, q_src), (k_raw, v_raw, q_raw)

    def peer(slot, row, col, where):
        side = row // half
        turn = slot + 1
        same = side * half + (row + turn // COLUMNS) % half
        away = (slot - near_side) // COLUMNS
        other = where(side == 0, half + away, half - 1 - away)
        is_near = slot < near_side
        shift = where(is_near, turn, slot - near_side)
        return where(is_near, same, other), (col + shift) % COLUMNS

    def pick(test, yes, no):
        return yes if test else no

    def distances(slot, chosen_rows):
        found = set()
        for r in chosen_rows:
            for c in range(COLUMNS):
                pr, pc = peer(slot, r, c, pick)
                found.add(abs(pr - r) + abs(pc - c))
        return sorted(found)

    def traced_peer(slot):
        pr, pc = peer(slot, row, col, jnp.where)
        return pr * COLUMNS + pc, jnp.abs(pr - row) + jnp.abs(pc - col)

    def rows_of(block):
        return pl.ds(pl.multiple_of(block * tokens, tokens), tokens)

    def cols_of(head):
        return pl.ds(pl.multiple_of(head * HEAD_DIM, HEAD_DIM), HEAD_DIM)

    def in_copy(head, which, target, source, other):
        return pltpu.make_async_remote_copy(
            src_ref=refs[which].at[:, :, cols_of(target * heads + head)],
            dst_ref=raws[which].at[head, rows_of(source)],
            send_sem=in_send,
            recv_sem=in_recv.at[head * 3 + which, source],
            device_id=(other, me_i),
            device_id_type=MESH,
        )

    def send_in(head, which, other):
        in_copy(head, which, other, me_o, other).start()

    def wait_in(head, which, source):
        in_copy(head, which, me_o, source, source).wait_recv()

    def own_copy(head, which):
        return pltpu.make_async_copy(
            refs[which].at[:, :, cols_of(me_o * heads + head)],
            raws[which].at[head, rows_of(me_o)],
            local_sem.at[head * 3 + which],
        )

    def out_cols(source_o, source_i, head):
        return cols_of(source_i * (local_cols // HEAD_DIM) + source_o * heads + head)

    def out_slice(block, part):
        return pl.ds(block * tokens + part * out_rows, out_rows)

    def out_copy(head, block, part):
        return pltpu.make_async_remote_copy(
            src_ref=o_raw.at[head, out_slice(block, part)],
            dst_ref=out_ref.at[:, :, out_cols(me_o, me_i, head)],
            send_sem=out_send,
            recv_sem=out_recv,
            device_id=(block, part),
            device_id_type=MESH,
        )

    def out_own(head):
        return pltpu.make_async_copy(
            o_raw.at[head, out_slice(me_o, me_i)],
            out_ref.at[:, :, out_cols(me_o, me_i, head)],
            out_recv,
        )

    def tell(sem, device):
        pl.semaphore_signal(sem, inc=1, device_id=device, device_id_type=MESH)

    beside = [
        (row > 0, me_o - COLUMNS),
        (row < rows - 1, me_o + COLUMNS),
        (col > 0, me_o - 1),
        (col < COLUMNS - 1, me_o + 1),
    ]
    beside_count = sum(jnp.where(exists, 1, 0) for exists, other in beside)

    def tell_beside(sem):
        for exists, other in beside:
            @pl.when(exists)
            def _():
                tell(sem, (other, me_i))

    def meet(round_at):
        tell_beside(ready.at[round_at])
        pl.semaphore_wait(ready.at[round_at], beside_count)

    barrier = pltpu.get_barrier_semaphore()
    tell_beside(barrier)
    for shift in range(1, inner):
        tell(barrier, (me_o, (me_i + shift) % inner))
    sources = [
        pltpu.make_async_copy(ref, kept, src_sem.at[which])
        for which, (ref, kept) in enumerate(zip((k_ref, v_ref, q_ref), refs))
    ]
    for copy in sources:
        copy.start()
    for copy in sources:
        copy.wait()
    pl.semaphore_wait(barrier, beside_count + inner - 1)

    near_slots, away_slots = range(near_side), range(near_side, outer - 1)
    central = jnp.abs(2 * row - (rows - 1)) == 1
    central_rows = (half - 1, half)
    outward_rows = [r for r in range(rows) if r not in central_rows]
    furthest = rows + COLUMNS - 2

    def send_at(reach, slots, sent, chosen_rows, chosen=None):
        for slot in slots:
            lengths = distances(slot, chosen_rows)
            if reach not in lengths:
                continue
            other, length = traced_peer(slot)
            test = chosen
            if len(lengths) > 1:
                near_enough = length == reach
                test = near_enough if test is None else jnp.logical_and(test, near_enough)

            def send():
                for which in sent:
                    send_in(0, which, other)

            if test is None:
                send()
            else:
                pl.when(test)(send)

    def send_queries(head):
        for slot in away_slots:
            send_in(head, 2, traced_peer(slot)[0])

    outward = jnp.logical_not(central)
    for reach in range(1, furthest + 1):
        if reach > 1:
            meet(reach - 2)
        send_at(reach, away_slots, (0, 1), central_rows, central)
        send_at(reach, near_slots, (0, 1, 2), range(rows))
        send_at(reach, away_slots, (0, 1), outward_rows, outward)
    pl.when(outward)(partial(send_queries, 0))
    for head in range(heads):
        for which in range(3):
            own_copy(head, which).start()
            for slot in range(outer - 1) if head else ():
                send_in(head, which, traced_peer(slot)[0])
    meet(furthest - 1)

    both = networks * tokens
    split_row = lax.broadcasted_iota(jnp.int32, (both, both), 0)
    split_col = lax.broadcasted_iota(jnp.int32, (both, both), 1)
    split = (split_col == (split_row % tokens) * networks + split_row // tokens)
    split = split.astype(jnp.float32).astype(jnp.bfloat16)
    join = (split_row == (split_col % tokens) * networks + split_col // tokens)
    join = join.astype(jnp.float32).astype(jnp.bfloat16)

    def separate(raw, head, block):
        mixed = raw[head, rows_of(block)].reshape(both, HEAD_DIM)
        return jnp.dot(split, mixed, preferred_element_type=jnp.float32).astype(jnp.bfloat16)

    def place(head, which, block):
        apart = separate(raws[which], head, block)
        kept = (k_buf, v_buf)[which]
        for network in range(networks):
            kept[network, rows_of(block)] = apart[network * tokens:(network + 1) * tokens]

    def compute(head, block):
        query = separate(q_raw, head, block)
        parts = [
            attend_block(query[n * tokens:(n + 1) * tokens], k_buf[n], v_buf[n])
            for n in range(networks)
        ]
        mixed = jnp.dot(join, jnp.concatenate(parts, axis=0), preferred_element_type=jnp.float32)
        o_raw[head, rows_of(block)] = mixed.astype(jnp.bfloat16).reshape(
            tokens, networks, HEAD_DIM
        )

    for head in range(heads):
        for which in range(3):
            own_copy(head, which).wait()
        for which in range(2):
            place(head, which, me_o)

        def one_place(slot, carry):
            block = traced_peer(slot)[0]
            for which in range(2):
                wait_in(head, which, block)
                place(head, which, block)
            return carry

        lax.fori_loop(0, outer - 1, one_place, 0)
        if head == 0:
            pl.when(central)(partial(send_queries, 0))

        compute(head, me_o)
        for shift in range(1, inner):
            out_copy(head, me_o, (me_i + shift) % inner).start()
        out_own(head).start()

        def one_block(index, carry):
            slot = jnp.where(index < near_side, index, outer - 2 + near_side - index)
            block = traced_peer(slot)[0]
            wait_in(head, 2, block)
            compute(head, block)
            for part in range(inner):
                out_copy(head, block, part).start()
            return carry

        lax.fori_loop(0, outer - 1, one_block, 0)

    def wait_bytes(ref, sem):
        pltpu.make_async_copy(ref, ref, sem).wait()

    for head in range(heads):
        for raw in raws:
            wait_bytes(raw.at[head, pl.ds(0, tokens * (outer - 1))], in_send)
        wait_bytes(o_raw.at[head, pl.ds(0, tokens * outer - out_rows)], out_send)
    wait_bytes(out_ref, out_recv)


def per_device(outer, inner, queries, keys, values):
    tokens, networks, local_cols = queries.shape
    heads = local_cols // HEAD_DIM // outer
    seq = tokens * outer
    out_rows = tokens // inner
    raw = pltpu.VMEM((heads, seq, networks, HEAD_DIM), jnp.bfloat16)
    kept = pltpu.VMEM((networks, seq, HEAD_DIM), jnp.bfloat16)
    return pl.pallas_call(
        partial(exchange_kernel, outer, inner, heads),
        out_shape=jax.ShapeDtypeStruct((out_rows, networks, local_cols * inner), jnp.bfloat16),
        in_specs=[pl.BlockSpec(memory_space=pl.ANY)] * 3,
        out_specs=pl.BlockSpec(memory_space=pl.ANY),
        scratch_shapes=[
            raw, raw, raw, kept, kept, raw,
            *[pltpu.VMEM(queries.shape, jnp.bfloat16)] * 3,
            pltpu.SemaphoreType.DMA((3,)),
            pltpu.SemaphoreType.DMA((heads * 3,)),
            pltpu.SemaphoreType.DMA,
            pltpu.SemaphoreType.DMA((heads * 3, outer)),
            pltpu.SemaphoreType.DMA,
            pltpu.SemaphoreType.DMA,
            pltpu.SemaphoreType.REGULAR((outer // COLUMNS + COLUMNS - 2,)),
        ],
        compiler_params=pltpu.CompilerParams(collective_id=0, has_side_effects=True, vmem_limit_bytes=54500 * 1024),
    )(queries, keys, values)


def solution(mesh):
    outer, inner = mesh.shape["outer"], mesh.shape["inner"]

    def body(queries, keys, values):
        heads = queries.shape[2] // HEAD_DIM
        if outer % (2 * COLUMNS) == 0 and heads % outer == 0:
            return per_device(outer, inner, queries, keys, values)
        return per_device_split(queries, keys, values)

    return jax.shard_map(
        body,
        mesh=mesh,
        in_specs=(P("outer", None, "inner"),) * 3,
        out_specs=P(("outer", "inner"), None, None),
        check_vma=False,
    )
```

```python
from functools import partial
import math

import jax
import jax.numpy as jnp
from jax import lax
from jax.experimental import pallas as pl
from jax.experimental.pallas import tpu as pltpu
from jax.sharding import PartitionSpec as P

HEAD_DIM = 128
MESH = pl.DeviceIdType.MESH


def attend_keys(running, key_block, value_block, query_heads, head_count):
    peak_rows, totals, numerator = running
    key_count = key_block.shape[0]
    key_heads = key_block.reshape(key_count, head_count, HEAD_DIM)
    value_heads = value_block.reshape(key_count, head_count, HEAD_DIM)
    scores = jnp.einsum(
        "qhd,khd->qhk", query_heads, key_heads, preferred_element_type=jnp.float32
    ) * (1.0 / math.sqrt(HEAD_DIM))
    new_peaks = jnp.maximum(peak_rows, jnp.max(scores, axis=2))
    shrink = jnp.exp(peak_rows - new_peaks)
    weights = jnp.exp(scores - new_peaks[..., None])
    totals = totals * shrink + jnp.sum(weights, axis=2)
    numerator = numerator * shrink[..., None] + jnp.einsum(
        "qhk,khd->qhd",
        weights.astype(jnp.bfloat16),
        value_heads,
        preferred_element_type=jnp.float32,
    )
    return (new_peaks, totals, numerator)


def attend_piece(running, pieces, query_part, head_count):
    key_rows, value_rows = pieces
    row_count = query_part.shape[0]
    query_heads = query_part.reshape(row_count, head_count, HEAD_DIM)
    block_count = key_rows.shape[0] // row_count
    key_blocks = key_rows.reshape(block_count, row_count, key_rows.shape[1])
    value_blocks = value_rows.reshape(block_count, row_count, value_rows.shape[1])

    def one_block(state, blocks):
        return (attend_keys(state, blocks[0], blocks[1], query_heads, head_count), None)

    running, unused = lax.scan(one_block, running, (key_blocks, value_blocks))
    return running


def start_state(row_count, head_count):
    peak_rows = jnp.full((row_count, head_count), -jnp.inf, jnp.float32)
    totals = jnp.zeros((row_count, head_count), jnp.float32)
    numerator = jnp.zeros((row_count, head_count, HEAD_DIM), jnp.float32)
    return (peak_rows, totals, numerator)


def finish_state(running):
    peak_rows, totals, numerator = running
    averaged = numerator / totals[..., None]
    return averaged.reshape(numerator.shape[0], -1).astype(jnp.bfloat16)


def flatten(array):
    return array.reshape(array.shape[0], array.shape[1] * array.shape[2])


def per_device_split(queries, keys, values):
    tok_rows, networks, local_cols = queries.shape
    full_q, full_k, full_v = (
        lax.all_to_all(array, "inner", split_axis=0, concat_axis=2, tiled=True)
        for array in (queries, keys, values)
    )
    unit_rows = full_q.shape[0]
    full_cols = full_q.shape[2]
    query_part, key_part, value_part = (
        lax.all_to_all(flatten(array), "outer", split_axis=1, concat_axis=0, tiled=True)
        for array in (full_q, full_k, full_v)
    )
    head_count = query_part.shape[1] // HEAD_DIM
    running = attend_piece(
        start_state(query_part.shape[0], head_count),
        (
            lax.all_gather(key_part, "inner", axis=0, tiled=True),
            lax.all_gather(value_part, "inner", axis=0, tiled=True),
        ),
        query_part,
        head_count,
    )
    gathered = lax.all_to_all(
        finish_state(running), "outer", split_axis=0, concat_axis=1, tiled=True
    )
    return gathered.reshape(unit_rows, networks, full_cols)


def attend_block(query, key, value):
    raw = lax.dot_general(
        query, key, (((1,), (1,)), ((), ())), preferred_element_type=jnp.float32
    )
    peak = jnp.max(raw, axis=1, keepdims=True)
    weights = jnp.exp2((raw - peak) * (math.log2(math.e) / math.sqrt(HEAD_DIM)))
    totals = jnp.sum(weights, axis=1, keepdims=True)
    numerator = jnp.dot(
        weights.astype(jnp.bfloat16), value, preferred_element_type=jnp.float32
    )
    return (numerator / totals).astype(jnp.bfloat16)


COLUMNS = 2


def exchange_kernel(
    outer, inner, heads,
    q_ref, k_ref, v_ref, out_ref,
    q_raw, k_raw, v_raw, k_buf, v_buf, o_raw,
    q_src, k_src, v_src, src_sem, local_sem, in_send, in_recv, out_send, out_recv, answer, ready,
):
    me_o, me_i = lax.axis_index("outer"), lax.axis_index("inner")
    tokens, networks, local_cols = q_ref.shape
    out_rows = out_ref.shape[0]
    rows, half = outer // COLUMNS, outer // COLUMNS // 2
    row, col = me_o // COLUMNS, me_o % COLUMNS
    near_side = half * COLUMNS - 1
    furthest = rows + COLUMNS - 2
    refs, raws = (k_src, v_src, q_src), (k_raw, v_raw, q_raw)

    def peer(slot, row, col, where):
        side = row // half
        turn = slot + 1
        same = side * half + (row + turn // COLUMNS) % half
        away = (slot - near_side) // COLUMNS
        other = where(side == 0, half + away, half - 1 - away)
        is_near = slot < near_side
        shift = where(is_near, turn, slot - near_side)
        return where(is_near, same, other), (col + shift) % COLUMNS

    def pick(test, yes, no):
        return yes if test else no

    def distances(slot, chosen_rows):
        found = set()
        for r in chosen_rows:
            for c in range(COLUMNS):
                pr, pc = peer(slot, r, c, pick)
                found.add(abs(pr - r) + abs(pc - c))
        return sorted(found)

    def traced_peer(slot):
        pr, pc = peer(slot, row, col, jnp.where)
        return pr * COLUMNS + pc, jnp.abs(pr - row) + jnp.abs(pc - col)

    def rows_of(block):
        return pl.ds(pl.multiple_of(block * tokens, tokens), tokens)

    def cols_of(head):
        return pl.ds(pl.multiple_of(head * HEAD_DIM, HEAD_DIM), HEAD_DIM)

    def in_copy(head, which, target, source, other):
        return pltpu.make_async_remote_copy(
            src_ref=refs[which].at[:, :, cols_of(target * heads + head)],
            dst_ref=raws[which].at[head, rows_of(source)],
            send_sem=in_send,
            recv_sem=in_recv.at[head * 3 + which, source],
            device_id=(other, me_i),
            device_id_type=MESH,
        )

    def send_in(head, which, other):
        in_copy(head, which, other, me_o, other).start()

    def wait_in(head, which, source):
        in_copy(head, which, me_o, source, source).wait_recv()

    def own_copy(head, which):
        return pltpu.make_async_copy(
            refs[which].at[:, :, cols_of(me_o * heads + head)],
            raws[which].at[head, rows_of(me_o)],
            local_sem.at[head * 3 + which],
        )

    def out_cols(source_o, source_i, head):
        return cols_of(source_i * (local_cols // HEAD_DIM) + source_o * heads + head)

    def out_slice(block, part):
        return pl.ds(block * tokens + part * out_rows, out_rows)

    def out_copy(head, block, part):
        return pltpu.make_async_remote_copy(
            src_ref=o_raw.at[head, out_slice(block, part)],
            dst_ref=out_ref.at[:, :, out_cols(me_o, me_i, head)],
            send_sem=out_send,
            recv_sem=out_recv,
            device_id=(block, part),
            device_id_type=MESH,
        )

    def out_own(head):
        return pltpu.make_async_copy(
            o_raw.at[head, out_slice(me_o, me_i)],
            out_ref.at[:, :, out_cols(me_o, me_i, head)],
            out_recv,
        )

    def tell(sem, device):
        pl.semaphore_signal(sem, inc=1, device_id=device, device_id_type=MESH)

    beside = [
        (row > 0, me_o - COLUMNS),
        (row < rows - 1, me_o + COLUMNS),
        (col > 0, me_o - 1),
        (col < COLUMNS - 1, me_o + 1),
    ]
    beside_count = sum(jnp.where(exists, 1, 0) for exists, other in beside)

    def tell_beside(sem):
        for exists, other in beside:
            @pl.when(exists)
            def _():
                tell(sem, (other, me_i))

    def meet(round_at):
        pl.semaphore_wait(ready.at[round_at], beside_count)
        if round_at < furthest - 1:
            tell_beside(ready.at[round_at + 1])

    sources = [
        pltpu.make_async_copy(ref, kept, src_sem.at[which])
        for which, (ref, kept) in enumerate(zip((k_ref, v_ref, q_ref), refs))
    ]
    barrier = pltpu.get_barrier_semaphore()
    facing = row + 1 == half
    greeted = [(row < rows - 1, (me_o + COLUMNS, me_i)), (col < COLUMNS - 1, (me_o + 1, me_i))]
    answered = [
        (jnp.logical_and(row > 0, row != half), (me_o - COLUMNS, me_i)),
        (col > 0, (me_o - 1, me_i)),
    ]
    for part in range(inner):
        greeted.append((part > me_i, (me_o, part)))
        answered.append((part < me_i, (me_o, part)))
    greeted.append((row == half, (me_o - COLUMNS, me_i)))

    def tell_those(sem, those):
        for exists, device in those:
            pl.when(exists)(partial(tell, sem, device))

    def count(*tests):
        return sum(jnp.where(test, 1, 0) for test in tests)

    def wait_for(sem, amount):
        pl.when(amount > 0)(lambda: pl.semaphore_wait(sem, amount))

    tell_those(barrier, greeted)
    for copy in sources:
        copy.start()
    wait_for(barrier, count(row > 0, col > 0, facing) + me_i)
    tell_those(answer, answered)
    near_slots, away_slots = range(near_side), range(near_side, outer - 1)
    central = jnp.abs(2 * row - (rows - 1)) == 1
    central_rows = (half - 1, half)
    outward_rows = [r for r in range(rows) if r not in central_rows]

    def send_at(reach, slots, sent, chosen_rows, chosen=None):
        for slot in slots:
            lengths = distances(slot, chosen_rows)
            if reach not in lengths:
                continue
            other, length = traced_peer(slot)
            test = chosen
            if len(lengths) > 1:
                near_enough = length == reach
                test = near_enough if test is None else jnp.logical_and(test, near_enough)

            def send():
                for which in sent:
                    send_in(0, which, other)

            if test is None:
                send()
            else:
                pl.when(test)(send)

    def send_queries(head, slots):
        for slot in slots:
            send_in(head, 2, traced_peer(slot)[0])

    outward = jnp.logical_not(central)
    facing_slot = (near_side,)
    away_slots_left = range(near_side + 1, outer - 1)
    for which in range(2):
        sources[which].wait()
        send_at(1, facing_slot, (which,), central_rows, central)
    sources[2].wait()
    above = jnp.logical_and(row < rows - 1, jnp.logical_not(facing))
    wait_for(answer, count(above, col < COLUMNS - 1) + inner - 1 - me_i)
    tell_beside(ready.at[0])
    for reach in range(1, furthest + 1):
        if reach > 1:
            meet(reach - 2)
        send_at(reach, away_slots_left, (0, 1), central_rows, central)
        send_at(reach, near_slots, (0, 1, 2), range(rows))
        send_at(reach, away_slots, (0, 1), outward_rows, outward)
    pl.when(outward)(partial(send_queries, 0, away_slots))
    for head in range(heads):
        for which in range(3):
            own_copy(head, which).start()
            for slot in range(outer - 1) if head else ():
                send_in(head, which, traced_peer(slot)[0])
    meet(furthest - 1)

    both = networks * tokens
    split_row = lax.broadcasted_iota(jnp.int32, (both, both), 0)
    split_col = lax.broadcasted_iota(jnp.int32, (both, both), 1)
    split = (split_col == (split_row % tokens) * networks + split_row // tokens)
    split = split.astype(jnp.float32).astype(jnp.bfloat16)
    join = (split_row == (split_col % tokens) * networks + split_col // tokens)
    join = join.astype(jnp.float32).astype(jnp.bfloat16)

    def separate(raw, head, block):
        mixed = raw[head, rows_of(block)].reshape(both, HEAD_DIM)
        return jnp.dot(split, mixed, preferred_element_type=jnp.float32).astype(jnp.bfloat16)

    def place(head, which, block):
        apart = separate(raws[which], head, block)
        kept = (k_buf, v_buf)[which]
        for network in range(networks):
            kept[network, rows_of(block)] = apart[network * tokens:(network + 1) * tokens]

    def compute(head, block):
        query = separate(q_raw, head, block)
        parts = [
            attend_block(query[n * tokens:(n + 1) * tokens], k_buf[n], v_buf[n])
            for n in range(networks)
        ]
        mixed = jnp.dot(join, jnp.concatenate(parts, axis=0), preferred_element_type=jnp.float32)
        o_raw[head, rows_of(block)] = mixed.astype(jnp.bfloat16).reshape(
            tokens, networks, HEAD_DIM
        )

    for head in range(heads):
        for which in range(3):
            own_copy(head, which).wait()
        for which in range(2):
            place(head, which, me_o)

        def one_place(slot, carry):
            block = traced_peer(slot)[0]
            for which in range(2):
                wait_in(head, which, block)
                place(head, which, block)
            return carry

        lax.fori_loop(0, outer - 1, one_place, 0)
        if head == 0:
            pl.when(central)(partial(send_queries, 0, away_slots))

        compute(head, me_o)
        for shift in range(1, inner):
            out_copy(head, me_o, (me_i + shift) % inner).start()
        out_own(head).start()

        def one_block(index, carry):
            slot = jnp.where(index < near_side, index, outer - 2 + near_side - index)
            block = traced_peer(slot)[0]
            wait_in(head, 2, block)
            compute(head, block)
            for part in range(inner):
                out_copy(head, block, part).start()
            return carry

        lax.fori_loop(0, outer - 1, one_block, 0)

    def wait_bytes(ref, sem):
        pltpu.make_async_copy(ref, ref, sem).wait()

    for head in range(heads):
        for raw in raws:
            wait_bytes(raw.at[head, pl.ds(0, tokens * (outer - 1))], in_send)
        wait_bytes(o_raw.at[head, pl.ds(0, tokens * outer - out_rows)], out_send)
    wait_bytes(out_ref, out_recv)


def per_device(outer, inner, queries, keys, values):
    tokens, networks, local_cols = queries.shape
    heads = local_cols // HEAD_DIM // outer
    seq = tokens * outer
    out_rows = tokens // inner
    raw = pltpu.VMEM((heads, seq, networks, HEAD_DIM), jnp.bfloat16)
    kept = pltpu.VMEM((networks, seq, HEAD_DIM), jnp.bfloat16)
    return pl.pallas_call(
        partial(exchange_kernel, outer, inner, heads),
        out_shape=jax.ShapeDtypeStruct((out_rows, networks, local_cols * inner), jnp.bfloat16),
        in_specs=[pl.BlockSpec(memory_space=pl.ANY)] * 3,
        out_specs=pl.BlockSpec(memory_space=pl.ANY),
        scratch_shapes=[
            raw, raw, raw, kept, kept, raw,
            *[pltpu.VMEM(queries.shape, jnp.bfloat16)] * 3,
            pltpu.SemaphoreType.DMA((3,)),
            pltpu.SemaphoreType.DMA((heads * 3,)),
            pltpu.SemaphoreType.DMA,
            pltpu.SemaphoreType.DMA((heads * 3, outer)),
            pltpu.SemaphoreType.DMA,
            pltpu.SemaphoreType.DMA,
            pltpu.SemaphoreType.REGULAR,
            pltpu.SemaphoreType.REGULAR((outer // COLUMNS + COLUMNS - 2,)),
        ],
        compiler_params=pltpu.CompilerParams(collective_id=0, has_side_effects=True, vmem_limit_bytes=54500 * 1024),
    )(queries, keys, values)


def solution(mesh):
    outer, inner = mesh.shape["outer"], mesh.shape["inner"]

    def body(queries, keys, values):
        heads = queries.shape[2] // HEAD_DIM
        if outer % (2 * COLUMNS) == 0 and heads % outer == 0:
            return per_device(outer, inner, queries, keys, values)
        return per_device_split(queries, keys, values)

    return jax.shard_map(
        body,
        mesh=mesh,
        in_specs=(P("outer", None, "inner"),) * 3,
        out_specs=P(("outer", "inner"), None, None),
        check_vma=False,
    )
```

```python
from functools import partial
import math

import jax
import jax.numpy as jnp
from jax import lax
from jax.experimental import pallas as pl
from jax.experimental.pallas import tpu as pltpu
from jax.sharding import PartitionSpec as P

HEAD_DIM = 128
MESH = pl.DeviceIdType.MESH


def attend_keys(running, key_block, value_block, query_heads, head_count):
    peak_rows, totals, numerator = running
    key_count = key_block.shape[0]
    key_heads = key_block.reshape(key_count, head_count, HEAD_DIM)
    value_heads = value_block.reshape(key_count, head_count, HEAD_DIM)
    scores = jnp.einsum(
        "qhd,khd->qhk", query_heads, key_heads, preferred_element_type=jnp.float32
    ) * (1.0 / math.sqrt(HEAD_DIM))
    new_peaks = jnp.maximum(peak_rows, jnp.max(scores, axis=2))
    shrink = jnp.exp(peak_rows - new_peaks)
    weights = jnp.exp(scores - new_peaks[..., None])
    totals = totals * shrink + jnp.sum(weights, axis=2)
    numerator = numerator * shrink[..., None] + jnp.einsum(
        "qhk,khd->qhd",
        weights.astype(jnp.bfloat16),
        value_heads,
        preferred_element_type=jnp.float32,
    )
    return (new_peaks, totals, numerator)


def attend_piece(running, pieces, query_part, head_count):
    key_rows, value_rows = pieces
    row_count = query_part.shape[0]
    query_heads = query_part.reshape(row_count, head_count, HEAD_DIM)
    block_count = key_rows.shape[0] // row_count
    key_blocks = key_rows.reshape(block_count, row_count, key_rows.shape[1])
    value_blocks = value_rows.reshape(block_count, row_count, value_rows.shape[1])

    def one_block(state, blocks):
        return (attend_keys(state, blocks[0], blocks[1], query_heads, head_count), None)

    running, unused = lax.scan(one_block, running, (key_blocks, value_blocks))
    return running


def start_state(row_count, head_count):
    peak_rows = jnp.full((row_count, head_count), -jnp.inf, jnp.float32)
    totals = jnp.zeros((row_count, head_count), jnp.float32)
    numerator = jnp.zeros((row_count, head_count, HEAD_DIM), jnp.float32)
    return (peak_rows, totals, numerator)


def finish_state(running):
    peak_rows, totals, numerator = running
    averaged = numerator / totals[..., None]
    return averaged.reshape(numerator.shape[0], -1).astype(jnp.bfloat16)


def flatten(array):
    return array.reshape(array.shape[0], array.shape[1] * array.shape[2])


def per_device_split(queries, keys, values):
    tok_rows, networks, local_cols = queries.shape
    full_q, full_k, full_v = (
        lax.all_to_all(array, "inner", split_axis=0, concat_axis=2, tiled=True)
        for array in (queries, keys, values)
    )
    unit_rows = full_q.shape[0]
    full_cols = full_q.shape[2]
    query_part, key_part, value_part = (
        lax.all_to_all(flatten(array), "outer", split_axis=1, concat_axis=0, tiled=True)
        for array in (full_q, full_k, full_v)
    )
    head_count = query_part.shape[1] // HEAD_DIM
    running = attend_piece(
        start_state(query_part.shape[0], head_count),
        (
            lax.all_gather(key_part, "inner", axis=0, tiled=True),
            lax.all_gather(value_part, "inner", axis=0, tiled=True),
        ),
        query_part,
        head_count,
    )
    gathered = lax.all_to_all(
        finish_state(running), "outer", split_axis=0, concat_axis=1, tiled=True
    )
    return gathered.reshape(unit_rows, networks, full_cols)


def attend_block(query, key, value):
    raw = lax.dot_general(
        query, key, (((1,), (1,)), ((), ())), preferred_element_type=jnp.float32
    )
    peak = jnp.max(raw, axis=1, keepdims=True)
    weights = jnp.exp2((raw - peak) * (math.log2(math.e) / math.sqrt(HEAD_DIM)))
    totals = jnp.sum(weights, axis=1, keepdims=True)
    numerator = jnp.dot(
        weights.astype(jnp.bfloat16), value, preferred_element_type=jnp.float32
    )
    return (numerator / totals).astype(jnp.bfloat16)


COLUMNS = 2


def exchange_kernel(
    outer, inner, heads,
    q_ref, k_ref, v_ref, out_ref,
    q_raw, k_raw, v_raw, k_buf, v_buf, o_raw,
    q_src, k_src, v_src, src_sem, local_sem, in_send, in_recv, out_send, out_recv, answer, ready,
):
    me_o, me_i = lax.axis_index("outer"), lax.axis_index("inner")
    tokens, networks, local_cols = q_ref.shape
    out_rows = out_ref.shape[0]
    rows, half = outer // COLUMNS, outer // COLUMNS // 2
    row, col = me_o // COLUMNS, me_o % COLUMNS
    near_side = half * COLUMNS - 1
    furthest = rows + COLUMNS - 2
    refs, raws = (k_src, v_src, q_src), (k_raw, v_raw, q_raw)

    def peer(slot, row, col, where):
        side = row // half
        turn = slot + 1
        same = side * half + (row + turn // COLUMNS) % half
        away = (slot - near_side) // COLUMNS
        other = where(side == 0, half + away, half - 1 - away)
        is_near = slot < near_side
        shift = where(is_near, turn, slot - near_side)
        return where(is_near, same, other), (col + shift) % COLUMNS

    def pick(test, yes, no):
        return yes if test else no

    def distances(slot, chosen_rows):
        found = set()
        for r in chosen_rows:
            for c in range(COLUMNS):
                pr, pc = peer(slot, r, c, pick)
                found.add(abs(pr - r) + abs(pc - c))
        return sorted(found)

    def traced_peer(slot):
        pr, pc = peer(slot, row, col, jnp.where)
        return pr * COLUMNS + pc, jnp.abs(pr - row) + jnp.abs(pc - col)

    def rows_of(block):
        return pl.ds(pl.multiple_of(block * tokens, tokens), tokens)

    def cols_of(head):
        return pl.ds(pl.multiple_of(head * HEAD_DIM, HEAD_DIM), HEAD_DIM)

    def in_copy(head, which, target, source, other):
        return pltpu.make_async_remote_copy(
            src_ref=refs[which].at[:, :, cols_of(target * heads + head)],
            dst_ref=raws[which].at[head, rows_of(source)],
            send_sem=in_send,
            recv_sem=in_recv.at[head * 3 + which, source],
            device_id=(other, me_i),
            device_id_type=MESH,
        )

    def send_in(head, which, other):
        in_copy(head, which, other, me_o, other).start()

    def wait_in(head, which, source):
        in_copy(head, which, me_o, source, source).wait_recv()

    def own_copy(head, which):
        return pltpu.make_async_copy(
            refs[which].at[:, :, cols_of(me_o * heads + head)],
            raws[which].at[head, rows_of(me_o)],
            local_sem.at[head * 3 + which],
        )

    def out_cols(source_o, source_i, head):
        return cols_of(source_i * (local_cols // HEAD_DIM) + source_o * heads + head)

    def out_slice(block, part):
        return pl.ds(block * tokens + part * out_rows, out_rows)

    def out_copy(head, block, part):
        return pltpu.make_async_remote_copy(
            src_ref=o_raw.at[head, out_slice(block, part)],
            dst_ref=out_ref.at[:, :, out_cols(me_o, me_i, head)],
            send_sem=out_send,
            recv_sem=out_recv,
            device_id=(block, part),
            device_id_type=MESH,
        )

    def out_own(head):
        return pltpu.make_async_copy(
            o_raw.at[head, out_slice(me_o, me_i)],
            out_ref.at[:, :, out_cols(me_o, me_i, head)],
            out_recv,
        )

    def tell(sem, device):
        pl.semaphore_signal(sem, inc=1, device_id=device, device_id_type=MESH)

    beside = [
        (row > 0, me_o - COLUMNS),
        (row < rows - 1, me_o + COLUMNS),
        (col > 0, me_o - 1),
        (col < COLUMNS - 1, me_o + 1),
    ]
    beside_count = sum(jnp.where(exists, 1, 0) for exists, other in beside)

    def tell_beside(sem):
        for exists, other in beside:
            @pl.when(exists)
            def _():
                tell(sem, (other, me_i))

    def meet(round_at):
        pl.semaphore_wait(ready.at[round_at], beside_count)
        if round_at < furthest - 1:
            tell_beside(ready.at[round_at + 1])

    sources = [
        pltpu.make_async_copy(ref, kept, src_sem.at[which])
        for which, (ref, kept) in enumerate(zip((k_ref, v_ref, q_ref), refs))
    ]
    barrier = pltpu.get_barrier_semaphore()
    facing = row + 1 == half
    greeted = [(row < rows - 1, (me_o + COLUMNS, me_i)), (col < COLUMNS - 1, (me_o + 1, me_i))]
    answered = [
        (jnp.logical_and(row > 0, row != half), (me_o - COLUMNS, me_i)),
        (col > 0, (me_o - 1, me_i)),
    ]
    for part in range(inner):
        greeted.append((part > me_i, (me_o, part)))
        answered.append((part < me_i, (me_o, part)))
    greeted.append((row == half, (me_o - COLUMNS, me_i)))

    def tell_those(sem, those):
        for exists, device in those:
            pl.when(exists)(partial(tell, sem, device))

    def count(*tests):
        return sum(jnp.where(test, 1, 0) for test in tests)

    def wait_for(sem, amount):
        pl.when(amount > 0)(lambda: pl.semaphore_wait(sem, amount))

    tell_those(barrier, greeted)
    for copy in sources:
        copy.start()
    wait_for(barrier, count(row > 0, col > 0, facing) + me_i)
    tell_those(answer, answered)
    away_slots = range(near_side, outer - 1)
    beside_slots = range(COLUMNS - 1)
    straight_slots = range(COLUMNS - 1, near_side, COLUMNS)
    turning_slots = [slot for slot in range(near_side) if slot not in straight_slots]
    corner_slots = turning_slots[COLUMNS - 1:]
    central = jnp.abs(2 * row - (rows - 1)) == 1
    central_rows = (half - 1, half)
    outward_rows = [r for r in range(rows) if r not in central_rows]

    def send_at(reach, slots, sent, chosen_rows, chosen, earliest=1):
        for slot in slots:
            lengths = distances(slot, chosen_rows)
            other, length = traced_peer(slot)

            def send():
                for which in sent:
                    send_in(0, which, other)

            for far in lengths:
                if max(far, min(earliest, furthest)) == reach:
                    whole = len(lengths) == 1
                    pl.when(chosen if whole else jnp.logical_and(chosen, length == far))(send)

    def send_queries(head, slots):
        for slot in slots:
            send_in(head, 2, traced_peer(slot)[0])

    outward = jnp.logical_not(central)
    away_slots_left = range(near_side + 1, outer - 1)
    for which in range(2):
        sources[which].wait()
        pl.when(central)(partial(send_in, 0, which, traced_peer(near_side)[0]))
    sources[2].wait()
    above = jnp.logical_and(row < rows - 1, jnp.logical_not(facing))
    wait_for(answer, count(above, col < COLUMNS - 1) + inner - 1 - me_i)
    tell_beside(ready.at[0])
    for reach in range(1, furthest + 1):
        if reach > 1:
            meet(reach - 2)
        send_at(reach, away_slots_left, (0, 1), central_rows, central)
        send_at(reach, straight_slots, (0, 1, 2), central_rows, central)
        send_at(reach, turning_slots, (0, 1, 2), central_rows, central, 3)
        send_at(reach, (*beside_slots, *straight_slots), (0, 1, 2), outward_rows, outward)
        send_at(reach, away_slots, (0, 1), outward_rows, outward)
        send_at(reach, corner_slots, (0, 1, 2), outward_rows, outward, 3)
    pl.when(outward)(partial(send_queries, 0, away_slots))
    for head in range(heads):
        for which in range(3):
            own_copy(head, which).start()
            for slot in range(outer - 1) if head else ():
                send_in(head, which, traced_peer(slot)[0])
    meet(furthest - 1)

    both = networks * tokens
    split_row = lax.broadcasted_iota(jnp.int32, (both, both), 0)
    split_col = lax.broadcasted_iota(jnp.int32, (both, both), 1)
    split = (split_col == (split_row % tokens) * networks + split_row // tokens)
    split = split.astype(jnp.float32).astype(jnp.bfloat16)
    join = (split_row == (split_col % tokens) * networks + split_col // tokens)
    join = join.astype(jnp.float32).astype(jnp.bfloat16)

    def separate(raw, head, block):
        mixed = raw[head, rows_of(block)].reshape(both, HEAD_DIM)
        return jnp.dot(split, mixed, preferred_element_type=jnp.float32).astype(jnp.bfloat16)

    def place(head, which, block):
        apart = separate(raws[which], head, block)
        kept = (k_buf, v_buf)[which]
        for network in range(networks):
            kept[network, rows_of(block)] = apart[network * tokens:(network + 1) * tokens]

    def compute(head, block):
        query = separate(q_raw, head, block)
        parts = [
            attend_block(query[n * tokens:(n + 1) * tokens], k_buf[n], v_buf[n])
            for n in range(networks)
        ]
        mixed = jnp.dot(join, jnp.concatenate(parts, axis=0), preferred_element_type=jnp.float32)
        o_raw[head, rows_of(block)] = mixed.astype(jnp.bfloat16).reshape(
            tokens, networks, HEAD_DIM
        )

    for head in range(heads):
        for which in range(3):
            own_copy(head, which).wait()
        for which in range(2):
            place(head, which, me_o)

        def one_place(slot, carry):
            block = traced_peer(slot)[0]
            for which in range(2):
                wait_in(head, which, block)
                place(head, which, block)
            return carry

        lax.fori_loop(0, outer - 1, one_place, 0)
        if head == 0:
            pl.when(central)(partial(send_queries, 0, away_slots))

        compute(head, me_o)
        for shift in range(1, inner):
            out_copy(head, me_o, (me_i + shift) % inner).start()
        out_own(head).start()

        def one_block(index, carry):
            slot = jnp.where(index < near_side, index, outer - 2 + near_side - index)
            block = traced_peer(slot)[0]
            wait_in(head, 2, block)
            compute(head, block)
            for part in range(inner):
                out_copy(head, block, part).start()
            return carry

        lax.fori_loop(0, outer - 1, one_block, 0)

    def wait_bytes(ref, sem):
        pltpu.make_async_copy(ref, ref, sem).wait()

    for head in range(heads):
        for raw in raws:
            wait_bytes(raw.at[head, pl.ds(0, tokens * (outer - 1))], in_send)
        wait_bytes(o_raw.at[head, pl.ds(0, tokens * outer - out_rows)], out_send)
    wait_bytes(out_ref, out_recv)


def per_device(outer, inner, queries, keys, values):
    tokens, networks, local_cols = queries.shape
    heads = local_cols // HEAD_DIM // outer
    seq = tokens * outer
    out_rows = tokens // inner
    raw = pltpu.VMEM((heads, seq, networks, HEAD_DIM), jnp.bfloat16)
    kept = pltpu.VMEM((networks, seq, HEAD_DIM), jnp.bfloat16)
    return pl.pallas_call(
        partial(exchange_kernel, outer, inner, heads),
        out_shape=jax.ShapeDtypeStruct((out_rows, networks, local_cols * inner), jnp.bfloat16),
        in_specs=[pl.BlockSpec(memory_space=pl.ANY)] * 3,
        out_specs=pl.BlockSpec(memory_space=pl.ANY),
        scratch_shapes=[
            raw, raw, raw, kept, kept, raw,
            *[pltpu.VMEM(queries.shape, jnp.bfloat16)] * 3,
            pltpu.SemaphoreType.DMA((3,)),
            pltpu.SemaphoreType.DMA((heads * 3,)),
            pltpu.SemaphoreType.DMA,
            pltpu.SemaphoreType.DMA((heads * 3, outer)),
            pltpu.SemaphoreType.DMA,
            pltpu.SemaphoreType.DMA,
            pltpu.SemaphoreType.REGULAR,
            pltpu.SemaphoreType.REGULAR((outer // COLUMNS + COLUMNS - 2,)),
        ],
        compiler_params=pltpu.CompilerParams(collective_id=0, has_side_effects=True, vmem_limit_bytes=54500 * 1024),
    )(queries, keys, values)


def solution(mesh):
    outer, inner = mesh.shape["outer"], mesh.shape["inner"]

    def body(queries, keys, values):
        heads = queries.shape[2] // HEAD_DIM
        if outer % (2 * COLUMNS) == 0 and heads % outer == 0:
            return per_device(outer, inner, queries, keys, values)
        return per_device_split(queries, keys, values)

    return jax.shard_map(
        body,
        mesh=mesh,
        in_specs=(P("outer", None, "inner"),) * 3,
        out_specs=P(("outer", "inner"), None, None),
        check_vma=False,
    )
```

```python
from functools import partial
import math

import jax
import jax.numpy as jnp
from jax import lax
from jax.experimental import pallas as pl
from jax.experimental.pallas import tpu as pltpu
from jax.sharding import PartitionSpec as P

HEAD_DIM = 128
MESH = pl.DeviceIdType.MESH


def attend_keys(running, key_block, value_block, query_heads, head_count):
    peak_rows, totals, numerator = running
    key_count = key_block.shape[0]
    key_heads = key_block.reshape(key_count, head_count, HEAD_DIM)
    value_heads = value_block.reshape(key_count, head_count, HEAD_DIM)
    scores = jnp.einsum(
        "qhd,khd->qhk", query_heads, key_heads, preferred_element_type=jnp.float32
    ) * (1.0 / math.sqrt(HEAD_DIM))
    new_peaks = jnp.maximum(peak_rows, jnp.max(scores, axis=2))
    shrink = jnp.exp(peak_rows - new_peaks)
    weights = jnp.exp(scores - new_peaks[..., None])
    totals = totals * shrink + jnp.sum(weights, axis=2)
    numerator = numerator * shrink[..., None] + jnp.einsum(
        "qhk,khd->qhd",
        weights.astype(jnp.bfloat16),
        value_heads,
        preferred_element_type=jnp.float32,
    )
    return (new_peaks, totals, numerator)


def attend_piece(running, pieces, query_part, head_count):
    key_rows, value_rows = pieces
    row_count = query_part.shape[0]
    query_heads = query_part.reshape(row_count, head_count, HEAD_DIM)
    block_count = key_rows.shape[0] // row_count
    key_blocks = key_rows.reshape(block_count, row_count, key_rows.shape[1])
    value_blocks = value_rows.reshape(block_count, row_count, value_rows.shape[1])

    def one_block(state, blocks):
        return (attend_keys(state, blocks[0], blocks[1], query_heads, head_count), None)

    running, unused = lax.scan(one_block, running, (key_blocks, value_blocks))
    return running


def start_state(row_count, head_count):
    peak_rows = jnp.full((row_count, head_count), -jnp.inf, jnp.float32)
    totals = jnp.zeros((row_count, head_count), jnp.float32)
    numerator = jnp.zeros((row_count, head_count, HEAD_DIM), jnp.float32)
    return (peak_rows, totals, numerator)


def finish_state(running):
    peak_rows, totals, numerator = running
    averaged = numerator / totals[..., None]
    return averaged.reshape(numerator.shape[0], -1).astype(jnp.bfloat16)


def flatten(array):
    return array.reshape(array.shape[0], array.shape[1] * array.shape[2])


def per_device_split(queries, keys, values):
    tok_rows, networks, local_cols = queries.shape
    full_q, full_k, full_v = (
        lax.all_to_all(array, "inner", split_axis=0, concat_axis=2, tiled=True)
        for array in (queries, keys, values)
    )
    unit_rows = full_q.shape[0]
    full_cols = full_q.shape[2]
    query_part, key_part, value_part = (
        lax.all_to_all(flatten(array), "outer", split_axis=1, concat_axis=0, tiled=True)
        for array in (full_q, full_k, full_v)
    )
    head_count = query_part.shape[1] // HEAD_DIM
    running = attend_piece(
        start_state(query_part.shape[0], head_count),
        (
            lax.all_gather(key_part, "inner", axis=0, tiled=True),
            lax.all_gather(value_part, "inner", axis=0, tiled=True),
        ),
        query_part,
        head_count,
    )
    gathered = lax.all_to_all(
        finish_state(running), "outer", split_axis=0, concat_axis=1, tiled=True
    )
    return gathered.reshape(unit_rows, networks, full_cols)


def attend_block(query, key, value):
    raw = lax.dot_general(
        query, key, (((1,), (1,)), ((), ())), preferred_element_type=jnp.float32
    )
    peak = jnp.max(raw, axis=1, keepdims=True)
    weights = jnp.exp2((raw - peak) * (math.log2(math.e) / math.sqrt(HEAD_DIM)))
    totals = jnp.sum(weights, axis=1, keepdims=True)
    numerator = jnp.dot(
        weights.astype(jnp.bfloat16), value, preferred_element_type=jnp.float32
    )
    return (numerator / totals).astype(jnp.bfloat16)


COLUMNS = 2
CORES = 2


def exchange_kernel(
    outer, inner, heads,
    q_ref, k_ref, v_ref, out_ref,
    q_raw, k_raw, v_raw, k_buf, v_buf, o_raw,
    q_src, k_src, v_src, src_sem, local_sem, in_send, in_recv, out_send, out_recv, answer, ready, first_src, first_sem,
):
    me_o, me_i = lax.axis_index("outer"), lax.axis_index("inner")
    tokens, networks, local_cols = q_ref.shape
    out_rows = out_ref.shape[0]
    rows, half = outer // COLUMNS, outer // COLUMNS // 2
    row, col = me_o // COLUMNS, me_o % COLUMNS
    near_side = half * COLUMNS - 1
    furthest = rows + COLUMNS - 2
    refs, raws = (k_src, v_src, q_src), (k_raw, v_raw, q_raw)

    def peer(slot, row, col, where):
        side = row // half
        turn = slot + 1
        same = side * half + (row + turn // COLUMNS) % half
        away = (slot - near_side) // COLUMNS
        other = where(side == 0, half + away, half - 1 - away)
        is_near = slot < near_side
        shift = where(is_near, turn, slot - near_side)
        return where(is_near, same, other), (col + shift) % COLUMNS

    def pick(test, yes, no):
        return yes if test else no

    def distances(slot, chosen_rows):
        found = set()
        for r in chosen_rows:
            for c in range(COLUMNS):
                pr, pc = peer(slot, r, c, pick)
                found.add(abs(pr - r) + abs(pc - c))
        return sorted(found)

    def traced_peer(slot):
        pr, pc = peer(slot, row, col, jnp.where)
        return pr * COLUMNS + pc, jnp.abs(pr - row) + jnp.abs(pc - col)

    def rows_of(block):
        return pl.ds(pl.multiple_of(block * tokens, tokens), tokens)

    def cols_of(head):
        return pl.ds(pl.multiple_of(head * HEAD_DIM, HEAD_DIM), HEAD_DIM)

    def in_copy(head, which, target, source, other):
        return pltpu.make_async_remote_copy(
            src_ref=refs[which].at[:, :, cols_of(target * heads + head)],
            dst_ref=raws[which].at[head, rows_of(source)],
            send_sem=in_send,
            recv_sem=in_recv.at[head * 3 + which, source],
            device_id=(other, me_i),
            device_id_type=MESH,
        )

    def send_in(head, which, other):
        in_copy(head, which, other, me_o, other).start()

    def wait_in(head, which, source):
        in_copy(head, which, me_o, source, source).wait_recv()

    def own_copy(head, which):
        return pltpu.make_async_copy(
            refs[which].at[:, :, cols_of(me_o * heads + head)],
            raws[which].at[head, rows_of(me_o)],
            local_sem.at[head * 3 + which],
        )

    def out_cols(source_o, source_i, head):
        return cols_of(source_i * (local_cols // HEAD_DIM) + source_o * heads + head)

    def out_slice(block, part):
        return pl.ds(block * tokens + part * out_rows, out_rows)

    def out_copy(head, block, part):
        return pltpu.make_async_remote_copy(
            src_ref=o_raw.at[head, out_slice(block, part)],
            dst_ref=out_ref.at[:, :, out_cols(me_o, me_i, head)],
            send_sem=out_send,
            recv_sem=out_recv,
            device_id=(block, part),
            device_id_type=MESH,
        )

    def out_own(head):
        return pltpu.make_async_copy(
            o_raw.at[head, out_slice(me_o, me_i)],
            out_ref.at[:, :, out_cols(me_o, me_i, head)],
            out_recv,
        )

    def tell(sem, device):
        pl.semaphore_signal(sem, inc=1, device_id=device, device_id_type=MESH)

    beside = [
        (row > 0, me_o - COLUMNS),
        (row < rows - 1, me_o + COLUMNS),
        (col > 0, me_o - 1),
        (col < COLUMNS - 1, me_o + 1),
    ]
    beside_count = sum(jnp.where(exists, 1, 0) for exists, other in beside)

    def tell_beside(sem):
        for exists, other in beside:
            @pl.when(exists)
            def _():
                tell(sem, (other, me_i))

    def meet(round_at):
        pl.semaphore_wait(ready.at[round_at], beside_count)
        if round_at < furthest - 1:
            tell_beside(ready.at[round_at + 1])

    sources = [
        pltpu.make_async_copy(ref, kept, src_sem.at[which])
        for which, (ref, kept) in enumerate(zip((k_ref, v_ref, q_ref), refs))
    ]
    barrier = pltpu.get_barrier_semaphore()
    facing = row + 1 == half
    greeted = [(row < rows - 1, (me_o + COLUMNS, me_i)), (col < COLUMNS - 1, (me_o + 1, me_i))]
    answered = [
        (jnp.logical_and(row > 0, row != half), (me_o - COLUMNS, me_i)),
        (col > 0, (me_o - 1, me_i)),
    ]
    for part in range(inner):
        greeted.append((part > me_i, (me_o, part)))
        answered.append((part < me_i, (me_o, part)))
    greeted.insert(0, (row == half, (me_o - COLUMNS, me_i)))

    def tell_those(sem, those):
        for exists, device in those:
            pl.when(exists)(partial(tell, sem, device))

    def count(*tests):
        return sum(jnp.where(test, 1, 0) for test in tests)

    def wait_for(sem, amount):
        pl.when(amount > 0)(lambda: pl.semaphore_wait(sem, amount))

    central = jnp.abs(2 * row - (rows - 1)) == 1
    facing_to = traced_peer(near_side)[0]
    firsts = [
        pltpu.make_async_copy(
            ref.at[:, :, cols_of(facing_to * heads)], first_src.at[which], first_sem.at[which]
        )
        for which, ref in enumerate((k_ref, v_ref))
    ]

    def each_first(act):
        for first in firsts:
            act(first)

    tell_those(barrier, greeted[:2])
    pl.when(central)(lambda: each_first(lambda first: first.start()))
    for copy in sources:
        copy.start()
    tell_those(barrier, greeted[2:])
    wait_for(barrier, count(row > 0, col > 0, facing) + me_i)
    tell_those(answer, answered)
    away_slots = range(near_side, outer - 1)
    beside_slots = range(COLUMNS - 1)
    straight_slots = range(COLUMNS - 1, near_side, COLUMNS)
    turning_slots = [slot for slot in range(near_side) if slot not in straight_slots]
    corner_slots = turning_slots[COLUMNS - 1:]
    central_rows = (half - 1, half)
    outward_rows = [r for r in range(rows) if r not in central_rows]

    def send_at(reach, slots, sent, chosen_rows, chosen, earliest=1):
        for slot in slots:
            lengths = distances(slot, chosen_rows)
            other, length = traced_peer(slot)

            def send():
                for which in sent:
                    send_in(0, which, other)

            for far in lengths:
                if max(far, min(earliest, furthest)) == reach:
                    whole = len(lengths) == 1
                    pl.when(chosen if whole else jnp.logical_and(chosen, length == far))(send)

    def send_queries(head, slots):
        for slot in slots:
            send_in(head, 2, traced_peer(slot)[0])

    outward = jnp.logical_not(central)
    away_slots_left = range(near_side + 1, outer - 1)
    def send_first():
        for which in range(2):
            firsts[which].wait()
            pltpu.make_async_remote_copy(
                src_ref=first_src.at[which],
                dst_ref=raws[which].at[0, rows_of(me_o)],
                send_sem=in_send,
                recv_sem=in_recv.at[which, me_o],
                device_id=(facing_to, me_i),
                device_id_type=MESH,
            ).start()

    pl.when(central)(send_first)
    for copy in sources:
        copy.wait()
    above = jnp.logical_and(row < rows - 1, jnp.logical_not(facing))
    wait_for(answer, count(above, col < COLUMNS - 1) + inner - 1 - me_i)
    tell_beside(ready.at[0])
    for reach in range(1, furthest + 1):
        if reach > 1:
            meet(reach - 2)
        send_at(reach, away_slots_left, (0, 1), central_rows, central)
        send_at(reach, straight_slots, (0, 1, 2), central_rows, central)
        send_at(reach, turning_slots, (0, 1, 2), central_rows, central, 3)
        send_at(reach, (*beside_slots, *straight_slots), (0, 1, 2), outward_rows, outward)
        send_at(reach, away_slots, (0, 1), outward_rows, outward)
        send_at(reach, corner_slots, (0, 1, 2), outward_rows, outward, 3)
    pl.when(outward)(partial(send_queries, 0, away_slots))
    for head in range(heads):
        for which in range(3):
            own_copy(head, which).start()
            for slot in range(outer - 1) if head else ():
                send_in(head, which, traced_peer(slot)[0])
    meet(furthest - 1)

    both = networks * tokens
    split_row = lax.broadcasted_iota(jnp.int32, (both, both), 0)
    split_col = lax.broadcasted_iota(jnp.int32, (both, both), 1)
    split = (split_col == (split_row % tokens) * networks + split_row // tokens)
    split = split.astype(jnp.float32).astype(jnp.bfloat16)
    join = (split_row == (split_col % tokens) * networks + split_col // tokens)
    join = join.astype(jnp.float32).astype(jnp.bfloat16)

    def separate(raw, head, block):
        mixed = raw[head, rows_of(block)].reshape(both, HEAD_DIM)
        return jnp.dot(split, mixed, preferred_element_type=jnp.float32).astype(jnp.bfloat16)

    def place(head, which, block):
        apart = separate(raws[which], head, block)
        kept = (k_buf, v_buf)[which]
        for network in range(networks):
            kept[network, rows_of(block)] = apart[network * tokens:(network + 1) * tokens]

    def compute(head, block):
        query = separate(q_raw, head, block)
        parts = [
            attend_block(query[n * tokens:(n + 1) * tokens], k_buf[n], v_buf[n])
            for n in range(networks)
        ]
        mixed = jnp.dot(join, jnp.concatenate(parts, axis=0), preferred_element_type=jnp.float32)
        o_raw[head, rows_of(block)] = mixed.astype(jnp.bfloat16).reshape(
            tokens, networks, HEAD_DIM
        )

    for head in range(heads):
        for which in range(3):
            own_copy(head, which).wait()
        for which in range(2):
            place(head, which, me_o)

        def one_place(slot, carry):
            block = traced_peer(slot)[0]
            for which in range(2):
                wait_in(head, which, block)
                place(head, which, block)
            return carry

        lax.fori_loop(0, outer - 1, one_place, 0)
        if head == 0:
            pl.when(central)(partial(send_queries, 0, away_slots))

        compute(head, me_o)
        for shift in range(1, inner):
            out_copy(head, me_o, (me_i + shift) % inner).start()
        out_own(head).start()

        def one_block(index, carry):
            slot = jnp.where(index < near_side, index, outer - 2 + near_side - index)
            block = traced_peer(slot)[0]
            wait_in(head, 2, block)
            compute(head, block)
            for turn in range(inner):
                chip = (me_i // CORES + 1 + turn // CORES) % (inner // CORES)
                core = (me_i + 1 + turn) % CORES
                out_copy(head, block, chip * CORES + core).start()
            return carry

        lax.fori_loop(0, outer - 1, one_block, 0)

    def wait_bytes(ref, sem):
        pltpu.make_async_copy(ref, ref, sem).wait()

    for head in range(heads):
        for raw in raws:
            wait_bytes(raw.at[head, pl.ds(0, tokens * (outer - 1))], in_send)
        wait_bytes(o_raw.at[head, pl.ds(0, tokens * outer - out_rows)], out_send)
    wait_bytes(out_ref, out_recv)


def per_device(outer, inner, queries, keys, values):
    tokens, networks, local_cols = queries.shape
    heads = local_cols // HEAD_DIM // outer
    seq = tokens * outer
    out_rows = tokens // inner
    raw = pltpu.VMEM((heads, seq, networks, HEAD_DIM), jnp.bfloat16)
    kept = pltpu.VMEM((networks, seq, HEAD_DIM), jnp.bfloat16)
    return pl.pallas_call(
        partial(exchange_kernel, outer, inner, heads),
        out_shape=jax.ShapeDtypeStruct((out_rows, networks, local_cols * inner), jnp.bfloat16),
        in_specs=[pl.BlockSpec(memory_space=pl.ANY)] * 3,
        out_specs=pl.BlockSpec(memory_space=pl.ANY),
        scratch_shapes=[
            raw, raw, raw, kept, kept, raw,
            *[pltpu.VMEM(queries.shape, jnp.bfloat16)] * 3,
            pltpu.SemaphoreType.DMA((3,)),
            pltpu.SemaphoreType.DMA((heads * 3,)),
            pltpu.SemaphoreType.DMA,
            pltpu.SemaphoreType.DMA((heads * 3, outer)),
            pltpu.SemaphoreType.DMA,
            pltpu.SemaphoreType.DMA,
            pltpu.SemaphoreType.REGULAR,
            pltpu.SemaphoreType.REGULAR((outer // COLUMNS + COLUMNS - 2,)),
            pltpu.VMEM((2, tokens, networks, HEAD_DIM), jnp.bfloat16),
            pltpu.SemaphoreType.DMA((2,)),
        ],
        compiler_params=pltpu.CompilerParams(collective_id=0, has_side_effects=True, vmem_limit_bytes=54500 * 1024),
    )(queries, keys, values)


def solution(mesh):
    outer, inner = mesh.shape["outer"], mesh.shape["inner"]

    def body(queries, keys, values):
        heads = queries.shape[2] // HEAD_DIM
        if outer % (2 * COLUMNS) == 0 and inner % CORES == 0 and heads % outer == 0:
            return per_device(outer, inner, queries, keys, values)
        return per_device_split(queries, keys, values)

    return jax.shard_map(
        body,
        mesh=mesh,
        in_specs=(P("outer", None, "inner"),) * 3,
        out_specs=P(("outer", "inner"), None, None),
        check_vma=False,
    )
```

```python
from functools import partial
import math

import jax
import jax.numpy as jnp
from jax import lax
from jax.experimental import pallas as pl
from jax.experimental.pallas import tpu as pltpu
from jax.sharding import PartitionSpec as P

HEAD_DIM = 128
MESH = pl.DeviceIdType.MESH


def attend_keys(running, key_block, value_block, query_heads, head_count):
    peak_rows, totals, numerator = running
    key_count = key_block.shape[0]
    key_heads = key_block.reshape(key_count, head_count, HEAD_DIM)
    value_heads = value_block.reshape(key_count, head_count, HEAD_DIM)
    scores = jnp.einsum(
        "qhd,khd->qhk", query_heads, key_heads, preferred_element_type=jnp.float32
    ) * (1.0 / math.sqrt(HEAD_DIM))
    new_peaks = jnp.maximum(peak_rows, jnp.max(scores, axis=2))
    shrink = jnp.exp(peak_rows - new_peaks)
    weights = jnp.exp(scores - new_peaks[..., None])
    totals = totals * shrink + jnp.sum(weights, axis=2)
    numerator = numerator * shrink[..., None] + jnp.einsum(
        "qhk,khd->qhd",
        weights.astype(jnp.bfloat16),
        value_heads,
        preferred_element_type=jnp.float32,
    )
    return (new_peaks, totals, numerator)


def attend_piece(running, pieces, query_part, head_count):
    key_rows, value_rows = pieces
    row_count = query_part.shape[0]
    query_heads = query_part.reshape(row_count, head_count, HEAD_DIM)
    block_count = key_rows.shape[0] // row_count
    key_blocks = key_rows.reshape(block_count, row_count, key_rows.shape[1])
    value_blocks = value_rows.reshape(block_count, row_count, value_rows.shape[1])

    def one_block(state, blocks):
        return (attend_keys(state, blocks[0], blocks[1], query_heads, head_count), None)

    running, unused = lax.scan(one_block, running, (key_blocks, value_blocks))
    return running


def start_state(row_count, head_count):
    peak_rows = jnp.full((row_count, head_count), -jnp.inf, jnp.float32)
    totals = jnp.zeros((row_count, head_count), jnp.float32)
    numerator = jnp.zeros((row_count, head_count, HEAD_DIM), jnp.float32)
    return (peak_rows, totals, numerator)


def finish_state(running):
    peak_rows, totals, numerator = running
    averaged = numerator / totals[..., None]
    return averaged.reshape(numerator.shape[0], -1).astype(jnp.bfloat16)


def flatten(array):
    return array.reshape(array.shape[0], array.shape[1] * array.shape[2])


def per_device_split(queries, keys, values):
    tok_rows, networks, local_cols = queries.shape
    full_q, full_k, full_v = (
        lax.all_to_all(array, "inner", split_axis=0, concat_axis=2, tiled=True)
        for array in (queries, keys, values)
    )
    unit_rows = full_q.shape[0]
    full_cols = full_q.shape[2]
    query_part, key_part, value_part = (
        lax.all_to_all(flatten(array), "outer", split_axis=1, concat_axis=0, tiled=True)
        for array in (full_q, full_k, full_v)
    )
    head_count = query_part.shape[1] // HEAD_DIM
    running = attend_piece(
        start_state(query_part.shape[0], head_count),
        (
            lax.all_gather(key_part, "inner", axis=0, tiled=True),
            lax.all_gather(value_part, "inner", axis=0, tiled=True),
        ),
        query_part,
        head_count,
    )
    gathered = lax.all_to_all(
        finish_state(running), "outer", split_axis=0, concat_axis=1, tiled=True
    )
    return gathered.reshape(unit_rows, networks, full_cols)


def attend_block(query, key, value):
    raw = lax.dot_general(
        query, key, (((1,), (1,)), ((), ())), preferred_element_type=jnp.float32
    )
    peak = jnp.max(raw, axis=1, keepdims=True)
    weights = jnp.exp2((raw - peak) * (math.log2(math.e) / math.sqrt(HEAD_DIM)))
    totals = jnp.sum(weights, axis=1, keepdims=True)
    numerator = jnp.dot(
        weights.astype(jnp.bfloat16), value, preferred_element_type=jnp.float32
    )
    return (numerator / totals).astype(jnp.bfloat16)


COLUMNS = 2


def exchange_kernel(
    outer, inner, heads,
    q_ref, k_ref, v_ref, out_ref,
    q_raw, k_raw, v_raw, k_buf, v_buf, o_raw,
    q_src, k_src, v_src, src_sem, local_sem, in_send, in_recv, out_send, out_recv, answer, ready,
):
    me_o, me_i = lax.axis_index("outer"), lax.axis_index("inner")
    tokens, networks, local_cols = q_ref.shape
    out_rows = out_ref.shape[0]
    rows, half = outer // COLUMNS, outer // COLUMNS // 2
    row, col = me_o // COLUMNS, me_o % COLUMNS
    near_side = half * COLUMNS - 1
    furthest = rows + COLUMNS - 2
    refs, raws = (k_src, v_src, q_src), (k_raw, v_raw, q_raw)

    def peer(slot, row, col, where):
        side = row // half
        turn = slot + 1
        same = side * half + (row + turn // COLUMNS) % half
        away = (slot - near_side) // COLUMNS
        other = where(side == 0, half + away, half - 1 - away)
        is_near = slot < near_side
        shift = where(is_near, turn, slot - near_side)
        return where(is_near, same, other), (col + shift) % COLUMNS

    def pick(test, yes, no):
        return yes if test else no

    def distances(slot, chosen_rows):
        found = set()
        for r in chosen_rows:
            for c in range(COLUMNS):
                pr, pc = peer(slot, r, c, pick)
                found.add(abs(pr - r) + abs(pc - c))
        return sorted(found)

    def traced_peer(slot):
        pr, pc = peer(slot, row, col, jnp.where)
        return pr * COLUMNS + pc, jnp.abs(pr - row) + jnp.abs(pc - col)

    def rows_of(block):
        return pl.ds(pl.multiple_of(block * tokens, tokens), tokens)

    def cols_of(head):
        return pl.ds(pl.multiple_of(head * HEAD_DIM, HEAD_DIM), HEAD_DIM)

    def in_copy(head, which, target, source, other):
        return pltpu.make_async_remote_copy(
            src_ref=refs[which].at[:, :, cols_of(target * heads + head)],
            dst_ref=raws[which].at[head, rows_of(source)],
            send_sem=in_send,
            recv_sem=in_recv.at[head * 3 + which, source],
            device_id=(other, me_i),
            device_id_type=MESH,
        )

    def send_in(head, which, other):
        in_copy(head, which, other, me_o, other).start()

    def wait_in(head, which, source):
        in_copy(head, which, me_o, source, source).wait_recv()

    def own_copy(head, which):
        return pltpu.make_async_copy(
            refs[which].at[:, :, cols_of(me_o * heads + head)],
            raws[which].at[head, rows_of(me_o)],
            local_sem.at[head * 3 + which],
        )

    def out_cols(source_o, source_i, head):
        return cols_of(source_i * (local_cols // HEAD_DIM) + source_o * heads + head)

    def out_slice(block, part):
        return pl.ds(block * tokens + part * out_rows, out_rows)

    def out_copy(head, block, part):
        return pltpu.make_async_remote_copy(
            src_ref=o_raw.at[head, out_slice(block, part)],
            dst_ref=out_ref.at[:, :, out_cols(me_o, me_i, head)],
            send_sem=out_send,
            recv_sem=out_recv,
            device_id=(block, part),
            device_id_type=MESH,
        )

    def out_own(head):
        return pltpu.make_async_copy(
            o_raw.at[head, out_slice(me_o, me_i)],
            out_ref.at[:, :, out_cols(me_o, me_i, head)],
            out_recv,
        )

    def tell(sem, device):
        pl.semaphore_signal(sem, inc=1, device_id=device, device_id_type=MESH)

    beside = [
        (row > 0, me_o - COLUMNS),
        (row < rows - 1, me_o + COLUMNS),
        (col > 0, me_o - 1),
        (col < COLUMNS - 1, me_o + 1),
    ]
    beside_count = sum(jnp.where(exists, 1, 0) for exists, other in beside)

    def tell_beside(sem):
        for exists, other in beside:
            @pl.when(exists)
            def _():
                tell(sem, (other, me_i))

    def meet(round_at):
        pl.semaphore_wait(ready.at[round_at], beside_count)
        if round_at < furthest - 1:
            tell_beside(ready.at[round_at + 1])

    sources = [
        pltpu.make_async_copy(ref, kept, src_sem.at[which])
        for which, (ref, kept) in enumerate(zip((k_ref, v_ref, q_ref), refs))
    ]
    barrier = pltpu.get_barrier_semaphore()
    facing = row + 1 == half
    greeted = [(row < rows - 1, (me_o + COLUMNS, me_i)), (col < COLUMNS - 1, (me_o + 1, me_i))]
    answered = [
        (jnp.logical_and(row > 0, row != half), (me_o - COLUMNS, me_i)),
        (col > 0, (me_o - 1, me_i)),
    ]
    for part in range(inner):
        greeted.append((part > me_i, (me_o, part)))
        answered.append((part < me_i, (me_o, part)))
    greeted.append((row == half, (me_o - COLUMNS, me_i)))

    def tell_those(sem, those):
        for exists, device in those:
            pl.when(exists)(partial(tell, sem, device))

    def count(*tests):
        return sum(jnp.where(test, 1, 0) for test in tests)

    def wait_for(sem, amount):
        pl.when(amount > 0)(lambda: pl.semaphore_wait(sem, amount))

    tell_those(barrier, greeted)
    for copy in sources:
        copy.start()
    wait_for(barrier, count(row > 0, col > 0, facing) + me_i)
    tell_those(answer, answered)
    away_slots = range(near_side, outer - 1)
    beside_slots = range(COLUMNS - 1)
    straight_slots = range(COLUMNS - 1, near_side, COLUMNS)
    turning_slots = [slot for slot in range(near_side) if slot not in straight_slots]
    corner_slots = turning_slots[COLUMNS - 1:]
    central = jnp.abs(2 * row - (rows - 1)) == 1
    central_rows = (half - 1, half)
    outward_rows = [r for r in range(rows) if r not in central_rows]

    def send_at(reach, slots, sent, chosen_rows, chosen, earliest=1):
        for slot in slots:
            lengths = distances(slot, chosen_rows)
            other, length = traced_peer(slot)

            def send():
                for which in sent:
                    send_in(0, which, other)

            for far in lengths:
                if max(far, min(earliest, furthest)) == reach:
                    whole = len(lengths) == 1
                    pl.when(chosen if whole else jnp.logical_and(chosen, length == far))(send)

    def send_queries(head, slots):
        for first in slots[::COLUMNS]:
            for turned in reversed(range(COLUMNS)):
                send_in(head, 2, traced_peer(first + turned)[0])

    outward = jnp.logical_not(central)
    away_slots_left = range(near_side + 1, outer - 1)
    for which in range(2):
        sources[which].wait()
        pl.when(central)(partial(send_in, 0, which, traced_peer(near_side)[0]))
    sources[2].wait()
    above = jnp.logical_and(row < rows - 1, jnp.logical_not(facing))
    wait_for(answer, count(above, col < COLUMNS - 1) + inner - 1 - me_i)
    tell_beside(ready.at[0])
    for reach in range(1, furthest + 1):
        if reach > 1:
            meet(reach - 2)
        send_at(reach, away_slots_left, (0, 1), central_rows, central)
        send_at(reach, straight_slots, (0, 1, 2), central_rows, central)
        send_at(reach, turning_slots, (0, 1, 2), central_rows, central, 3)
        send_at(reach, (*beside_slots, *straight_slots), (0, 1, 2), outward_rows, outward)
        send_at(reach, away_slots, (0, 1), outward_rows, outward)
        send_at(reach, corner_slots, (0, 1, 2), outward_rows, outward, 3)
    pl.when(outward)(partial(send_queries, 0, away_slots))
    for head in range(heads):
        for which in range(3):
            own_copy(head, which).start()
            for slot in range(outer - 1) if head else ():
                send_in(head, which, traced_peer(slot)[0])
    meet(furthest - 1)

    both = networks * tokens
    split_row = lax.broadcasted_iota(jnp.int32, (both, both), 0)
    split_col = lax.broadcasted_iota(jnp.int32, (both, both), 1)
    split = (split_col == (split_row % tokens) * networks + split_row // tokens)
    split = split.astype(jnp.float32).astype(jnp.bfloat16)
    join = (split_row == (split_col % tokens) * networks + split_col // tokens)
    join = join.astype(jnp.float32).astype(jnp.bfloat16)

    def separate(raw, head, block):
        mixed = raw[head, rows_of(block)].reshape(both, HEAD_DIM)
        return jnp.dot(split, mixed, preferred_element_type=jnp.float32).astype(jnp.bfloat16)

    def place(head, which, block):
        apart = separate(raws[which], head, block)
        kept = (k_buf, v_buf)[which]
        for network in range(networks):
            kept[network, rows_of(block)] = apart[network * tokens:(network + 1) * tokens]

    def compute(head, block):
        query = separate(q_raw, head, block)
        parts = [
            attend_block(query[n * tokens:(n + 1) * tokens], k_buf[n], v_buf[n])
            for n in range(networks)
        ]
        mixed = jnp.dot(join, jnp.concatenate(parts, axis=0), preferred_element_type=jnp.float32)
        o_raw[head, rows_of(block)] = mixed.astype(jnp.bfloat16).reshape(
            tokens, networks, HEAD_DIM
        )

    for head in range(heads):
        for which in range(3):
            own_copy(head, which).wait()
        for which in range(2):
            place(head, which, me_o)

        def one_place(slot, carry):
            block = traced_peer(slot)[0]
            for which in range(2):
                wait_in(head, which, block)
                place(head, which, block)
            return carry

        lax.fori_loop(0, outer - 1, one_place, 0)
        if head == 0:
            pl.when(central)(partial(send_queries, 0, away_slots))

        compute(head, me_o)
        for shift in range(1, inner):
            out_copy(head, me_o, (me_i + shift) % inner).start()
        out_own(head).start()

        def one_block(index, carry):
            slot = jnp.where(index < near_side, index, outer - 2 + near_side - index)
            block = traced_peer(slot)[0]
            wait_in(head, 2, block)
            compute(head, block)
            for part in range(inner):
                out_copy(head, block, part).start()
            return carry

        lax.fori_loop(0, outer - 1, one_block, 0)

    def wait_bytes(ref, sem):
        pltpu.make_async_copy(ref, ref, sem).wait()

    for head in range(heads):
        for raw in raws:
            wait_bytes(raw.at[head, pl.ds(0, tokens * (outer - 1))], in_send)
        wait_bytes(o_raw.at[head, pl.ds(0, tokens * outer - out_rows)], out_send)
    wait_bytes(out_ref, out_recv)


def per_device(outer, inner, queries, keys, values):
    tokens, networks, local_cols = queries.shape
    heads = local_cols // HEAD_DIM // outer
    seq = tokens * outer
    out_rows = tokens // inner
    raw = pltpu.VMEM((heads, seq, networks, HEAD_DIM), jnp.bfloat16)
    kept = pltpu.VMEM((networks, seq, HEAD_DIM), jnp.bfloat16)
    return pl.pallas_call(
        partial(exchange_kernel, outer, inner, heads),
        out_shape=jax.ShapeDtypeStruct((out_rows, networks, local_cols * inner), jnp.bfloat16),
        in_specs=[pl.BlockSpec(memory_space=pl.ANY)] * 3,
        out_specs=pl.BlockSpec(memory_space=pl.ANY),
        scratch_shapes=[
            raw, raw, raw, kept, kept, raw,
            *[pltpu.VMEM(queries.shape, jnp.bfloat16)] * 3,
            pltpu.SemaphoreType.DMA((3,)),
            pltpu.SemaphoreType.DMA((heads * 3,)),
            pltpu.SemaphoreType.DMA,
            pltpu.SemaphoreType.DMA((heads * 3, outer)),
            pltpu.SemaphoreType.DMA,
            pltpu.SemaphoreType.DMA,
            pltpu.SemaphoreType.REGULAR,
            pltpu.SemaphoreType.REGULAR((outer // COLUMNS + COLUMNS - 2,)),
        ],
        compiler_params=pltpu.CompilerParams(collective_id=0, has_side_effects=True, vmem_limit_bytes=54500 * 1024),
    )(queries, keys, values)


def solution(mesh):
    outer, inner = mesh.shape["outer"], mesh.shape["inner"]

    def body(queries, keys, values):
        heads = queries.shape[2] // HEAD_DIM
        if outer % (2 * COLUMNS) == 0 and heads % outer == 0:
            return per_device(outer, inner, queries, keys, values)
        return per_device_split(queries, keys, values)

    return jax.shard_map(
        body,
        mesh=mesh,
        in_specs=(P("outer", None, "inner"),) * 3,
        out_specs=P(("outer", "inner"), None, None),
        check_vma=False,
    )
```

```python
from functools import partial
import math

import jax
import jax.numpy as jnp
from jax import lax
from jax.experimental import pallas as pl
from jax.experimental.pallas import tpu as pltpu
from jax.sharding import PartitionSpec as P

HEAD_DIM = 128
MESH = pl.DeviceIdType.MESH


def attend_keys(running, key_block, value_block, query_heads, head_count):
    peak_rows, totals, numerator = running
    key_count = key_block.shape[0]
    key_heads = key_block.reshape(key_count, head_count, HEAD_DIM)
    value_heads = value_block.reshape(key_count, head_count, HEAD_DIM)
    scores = jnp.einsum(
        "qhd,khd->qhk", query_heads, key_heads, preferred_element_type=jnp.float32
    ) * (1.0 / math.sqrt(HEAD_DIM))
    new_peaks = jnp.maximum(peak_rows, jnp.max(scores, axis=2))
    shrink = jnp.exp(peak_rows - new_peaks)
    weights = jnp.exp(scores - new_peaks[..., None])
    totals = totals * shrink + jnp.sum(weights, axis=2)
    numerator = numerator * shrink[..., None] + jnp.einsum(
        "qhk,khd->qhd",
        weights.astype(jnp.bfloat16),
        value_heads,
        preferred_element_type=jnp.float32,
    )
    return (new_peaks, totals, numerator)


def attend_piece(running, pieces, query_part, head_count):
    key_rows, value_rows = pieces
    row_count = query_part.shape[0]
    query_heads = query_part.reshape(row_count, head_count, HEAD_DIM)
    block_count = key_rows.shape[0] // row_count
    key_blocks = key_rows.reshape(block_count, row_count, key_rows.shape[1])
    value_blocks = value_rows.reshape(block_count, row_count, value_rows.shape[1])

    def one_block(state, blocks):
        return (attend_keys(state, blocks[0], blocks[1], query_heads, head_count), None)

    running, unused = lax.scan(one_block, running, (key_blocks, value_blocks))
    return running


def start_state(row_count, head_count):
    peak_rows = jnp.full((row_count, head_count), -jnp.inf, jnp.float32)
    totals = jnp.zeros((row_count, head_count), jnp.float32)
    numerator = jnp.zeros((row_count, head_count, HEAD_DIM), jnp.float32)
    return (peak_rows, totals, numerator)


def finish_state(running):
    peak_rows, totals, numerator = running
    averaged = numerator / totals[..., None]
    return averaged.reshape(numerator.shape[0], -1).astype(jnp.bfloat16)


def flatten(array):
    return array.reshape(array.shape[0], array.shape[1] * array.shape[2])


def per_device_split(queries, keys, values):
    tok_rows, networks, local_cols = queries.shape
    full_q, full_k, full_v = (
        lax.all_to_all(array, "inner", split_axis=0, concat_axis=2, tiled=True)
        for array in (queries, keys, values)
    )
    unit_rows = full_q.shape[0]
    full_cols = full_q.shape[2]
    query_part, key_part, value_part = (
        lax.all_to_all(flatten(array), "outer", split_axis=1, concat_axis=0, tiled=True)
        for array in (full_q, full_k, full_v)
    )
    head_count = query_part.shape[1] // HEAD_DIM
    running = attend_piece(
        start_state(query_part.shape[0], head_count),
        (
            lax.all_gather(key_part, "inner", axis=0, tiled=True),
            lax.all_gather(value_part, "inner", axis=0, tiled=True),
        ),
        query_part,
        head_count,
    )
    gathered = lax.all_to_all(
        finish_state(running), "outer", split_axis=0, concat_axis=1, tiled=True
    )
    return gathered.reshape(unit_rows, networks, full_cols)


def attend_block(query, key, value):
    raw = lax.dot_general(
        query, key, (((1,), (1,)), ((), ())), preferred_element_type=jnp.float32
    )
    peak = jnp.max(raw, axis=1, keepdims=True)
    weights = jnp.exp2((raw - peak) * (math.log2(math.e) / math.sqrt(HEAD_DIM)))
    totals = jnp.sum(weights, axis=1, keepdims=True)
    numerator = jnp.dot(
        weights.astype(jnp.bfloat16), value, preferred_element_type=jnp.float32
    )
    return (numerator / totals).astype(jnp.bfloat16)


COLUMNS = 2


def exchange_kernel(
    outer, inner, heads,
    q_ref, k_ref, v_ref, out_ref,
    q_raw, k_raw, v_raw, k_buf, v_buf, o_raw,
    q_src, k_src, v_src, src_sem, local_sem, in_send, in_recv, out_send, out_recv, answer, ready,
):
    me_o, me_i = lax.axis_index("outer"), lax.axis_index("inner")
    tokens, networks, local_cols = q_ref.shape
    out_rows = out_ref.shape[0]
    rows, half = outer // COLUMNS, outer // COLUMNS // 2
    row, col = me_o // COLUMNS, me_o % COLUMNS
    near_side = half * COLUMNS - 1
    furthest = rows + COLUMNS - 2
    refs, raws = (k_src, v_src, q_src), (k_raw, v_raw, q_raw)

    def peer(slot, row, col, where):
        side = row // half
        turn = slot + 1
        same = side * half + (row + turn // COLUMNS) % half
        away = (slot - near_side) // COLUMNS
        other = where(side == 0, half + away, half - 1 - away)
        is_near = slot < near_side
        shift = where(is_near, turn, slot - near_side)
        return where(is_near, same, other), (col + shift) % COLUMNS

    def pick(test, yes, no):
        return yes if test else no

    def distances(slot, chosen_rows):
        found = set()
        for r in chosen_rows:
            for c in range(COLUMNS):
                pr, pc = peer(slot, r, c, pick)
                found.add(abs(pr - r) + abs(pc - c))
        return sorted(found)

    def traced_peer(slot):
        pr, pc = peer(slot, row, col, jnp.where)
        return pr * COLUMNS + pc, jnp.abs(pr - row) + jnp.abs(pc - col)

    def rows_of(block):
        return pl.ds(pl.multiple_of(block * tokens, tokens), tokens)

    def cols_of(head):
        return pl.ds(pl.multiple_of(head * HEAD_DIM, HEAD_DIM), HEAD_DIM)

    def in_copy(head, which, target, source, other):
        return pltpu.make_async_remote_copy(
            src_ref=refs[which].at[:, :, cols_of(target * heads + head)],
            dst_ref=raws[which].at[head, rows_of(source)],
            send_sem=in_send,
            recv_sem=in_recv.at[head * 3 + which, source],
            device_id=(other, me_i),
            device_id_type=MESH,
        )

    def send_in(head, which, other):
        in_copy(head, which, other, me_o, other).start()

    def wait_in(head, which, source):
        in_copy(head, which, me_o, source, source).wait_recv()

    def own_copy(head, which):
        return pltpu.make_async_copy(
            refs[which].at[:, :, cols_of(me_o * heads + head)],
            raws[which].at[head, rows_of(me_o)],
            local_sem.at[head * 3 + which],
        )

    def out_cols(source_o, source_i, head):
        return cols_of(source_i * (local_cols // HEAD_DIM) + source_o * heads + head)

    def out_slice(block, part):
        return pl.ds(block * tokens + part * out_rows, out_rows)

    def out_copy(head, block, part):
        return pltpu.make_async_remote_copy(
            src_ref=o_raw.at[head, out_slice(block, part)],
            dst_ref=out_ref.at[:, :, out_cols(me_o, me_i, head)],
            send_sem=out_send,
            recv_sem=out_recv,
            device_id=(block, part),
            device_id_type=MESH,
        )

    def out_own(head):
        return pltpu.make_async_copy(
            o_raw.at[head, out_slice(me_o, me_i)],
            out_ref.at[:, :, out_cols(me_o, me_i, head)],
            out_recv,
        )

    def tell(sem, device):
        pl.semaphore_signal(sem, inc=1, device_id=device, device_id_type=MESH)

    beside = [
        (row > 0, me_o - COLUMNS),
        (row < rows - 1, me_o + COLUMNS),
        (col > 0, me_o - 1),
        (col < COLUMNS - 1, me_o + 1),
    ]
    beside_count = sum(jnp.where(exists, 1, 0) for exists, other in beside)

    def tell_beside(sem):
        for exists, other in beside:
            @pl.when(exists)
            def _():
                tell(sem, (other, me_i))

    def meet(round_at):
        pl.semaphore_wait(ready.at[round_at], beside_count)
        if round_at < furthest - 1:
            tell_beside(ready.at[round_at + 1])

    sources = [
        pltpu.make_async_copy(ref, kept, src_sem.at[which])
        for which, (ref, kept) in enumerate(zip((k_ref, v_ref, q_ref), refs))
    ]
    barrier = pltpu.get_barrier_semaphore()
    facing = row + 1 == half
    greeted = [(row < rows - 1, (me_o + COLUMNS, me_i)), (col < COLUMNS - 1, (me_o + 1, me_i))]
    answered = [
        (jnp.logical_and(row > 0, row != half), (me_o - COLUMNS, me_i)),
        (col > 0, (me_o - 1, me_i)),
    ]
    for part in range(inner):
        greeted.append((part > me_i, (me_o, part)))
        answered.append((part < me_i, (me_o, part)))
    greeted.insert(0, (row == half, (me_o - COLUMNS, me_i)))

    def tell_those(sem, those):
        for exists, device in those:
            pl.when(exists)(partial(tell, sem, device))

    def count(*tests):
        return sum(jnp.where(test, 1, 0) for test in tests)

    def wait_for(sem, amount):
        pl.when(amount > 0)(lambda: pl.semaphore_wait(sem, amount))

    tell_those(barrier, greeted[:2])
    for copy in sources:
        copy.start()
    tell_those(barrier, greeted[2:])
    wait_for(barrier, count(row > 0, col > 0, facing) + me_i)
    tell_those(answer, answered)
    away_slots = range(near_side, outer - 1)
    beside_slots = range(COLUMNS - 1)
    straight_slots = range(COLUMNS - 1, near_side, COLUMNS)
    turning_slots = [slot for slot in range(near_side) if slot not in straight_slots]
    corner_slots = turning_slots[COLUMNS - 1:]
    central = jnp.abs(2 * row - (rows - 1)) == 1
    central_rows = (half - 1, half)
    outward_rows = [r for r in range(rows) if r not in central_rows]

    def send_at(reach, slots, sent, chosen_rows, chosen, earliest=1):
        for slot in slots:
            lengths = distances(slot, chosen_rows)
            other, length = traced_peer(slot)

            def send():
                for which in sent:
                    send_in(0, which, other)

            for far in lengths:
                if max(far, min(earliest, furthest)) == reach:
                    whole = len(lengths) == 1
                    pl.when(chosen if whole else jnp.logical_and(chosen, length == far))(send)

    def send_queries(head, slots):
        for slot in slots:
            send_in(head, 2, traced_peer(slot)[0])

    outward = jnp.logical_not(central)
    away_slots_left = range(near_side + 1, outer - 1)
    for which in range(2):
        sources[which].wait()
        pl.when(central)(partial(send_in, 0, which, traced_peer(near_side)[0]))
    sources[2].wait()
    above = jnp.logical_and(row < rows - 1, jnp.logical_not(facing))
    wait_for(answer, count(above, col < COLUMNS - 1) + inner - 1 - me_i)
    tell_beside(ready.at[0])
    for reach in range(1, furthest + 1):
        if reach > 1:
            meet(reach - 2)
        send_at(reach, away_slots_left, (0, 1), central_rows, central)
        send_at(reach, straight_slots, (0, 1, 2), central_rows, central)
        send_at(reach, turning_slots, (0, 1, 2), central_rows, central, 3)
        send_at(reach, (*beside_slots, *straight_slots), (0, 1, 2), outward_rows, outward)
        send_at(reach, away_slots, (0, 1), outward_rows, outward)
        send_at(reach, corner_slots, (0, 1, 2), outward_rows, outward, 3)
    pl.when(outward)(partial(send_queries, 0, away_slots))
    for head in range(heads):
        for which in range(3):
            own_copy(head, which).start()
            for slot in range(outer - 1) if head else ():
                send_in(head, which, traced_peer(slot)[0])
    meet(furthest - 1)

    both = networks * tokens
    split_row = lax.broadcasted_iota(jnp.int32, (both, both), 0)
    split_col = lax.broadcasted_iota(jnp.int32, (both, both), 1)
    split = (split_col == (split_row % tokens) * networks + split_row // tokens)
    split = split.astype(jnp.float32).astype(jnp.bfloat16)
    join = (split_row == (split_col % tokens) * networks + split_col // tokens)
    join = join.astype(jnp.float32).astype(jnp.bfloat16)

    def separate(raw, head, block):
        mixed = raw[head, rows_of(block)].reshape(both, HEAD_DIM)
        return jnp.dot(split, mixed, preferred_element_type=jnp.float32).astype(jnp.bfloat16)

    def place(head, which, block):
        apart = separate(raws[which], head, block)
        kept = (k_buf, v_buf)[which]
        for network in range(networks):
            kept[network, rows_of(block)] = apart[network * tokens:(network + 1) * tokens]

    def compute(head, block):
        query = separate(q_raw, head, block)
        parts = [
            attend_block(query[n * tokens:(n + 1) * tokens], k_buf[n], v_buf[n])
            for n in range(networks)
        ]
        mixed = jnp.dot(join, jnp.concatenate(parts, axis=0), preferred_element_type=jnp.float32)
        o_raw[head, rows_of(block)] = mixed.astype(jnp.bfloat16).reshape(
            tokens, networks, HEAD_DIM
        )

    for head in range(heads):
        for which in range(3):
            own_copy(head, which).wait()
        for which in range(2):
            place(head, which, me_o)

        def one_place(slot, carry):
            block = traced_peer(slot)[0]
            for which in range(2):
                wait_in(head, which, block)
                place(head, which, block)
            return carry

        lax.fori_loop(0, outer - 1, one_place, 0)
        if head == 0:
            pl.when(central)(partial(send_queries, 0, away_slots))

        compute(head, me_o)
        for shift in range(1, inner):
            out_copy(head, me_o, (me_i + shift) % inner).start()
        out_own(head).start()

        def one_block(index, carry):
            slot = jnp.where(index < near_side, index, outer - 2 + near_side - index)
            block = traced_peer(slot)[0]
            wait_in(head, 2, block)
            compute(head, block)
            for part in range(inner):
                out_copy(head, block, part).start()
            return carry

        lax.fori_loop(0, outer - 1, one_block, 0)

    def wait_bytes(ref, sem):
        pltpu.make_async_copy(ref, ref, sem).wait()

    for head in range(heads):
        for raw in raws:
            wait_bytes(raw.at[head, pl.ds(0, tokens * (outer - 1))], in_send)
        wait_bytes(o_raw.at[head, pl.ds(0, tokens * outer - out_rows)], out_send)
    wait_bytes(out_ref, out_recv)


def per_device(outer, inner, queries, keys, values):
    tokens, networks, local_cols = queries.shape
    heads = local_cols // HEAD_DIM // outer
    seq = tokens * outer
    out_rows = tokens // inner
    raw = pltpu.VMEM((heads, seq, networks, HEAD_DIM), jnp.bfloat16)
    kept = pltpu.VMEM((networks, seq, HEAD_DIM), jnp.bfloat16)
    return pl.pallas_call(
        partial(exchange_kernel, outer, inner, heads),
        out_shape=jax.ShapeDtypeStruct((out_rows, networks, local_cols * inner), jnp.bfloat16),
        in_specs=[pl.BlockSpec(memory_space=pl.ANY)] * 3,
        out_specs=pl.BlockSpec(memory_space=pl.ANY),
        scratch_shapes=[
            raw, raw, raw, kept, kept, raw,
            *[pltpu.VMEM(queries.shape, jnp.bfloat16)] * 3,
            pltpu.SemaphoreType.DMA((3,)),
            pltpu.SemaphoreType.DMA((heads * 3,)),
            pltpu.SemaphoreType.DMA,
            pltpu.SemaphoreType.DMA((heads * 3, outer)),
            pltpu.SemaphoreType.DMA,
            pltpu.SemaphoreType.DMA,
            pltpu.SemaphoreType.REGULAR,
            pltpu.SemaphoreType.REGULAR((outer // COLUMNS + COLUMNS - 2,)),
        ],
        compiler_params=pltpu.CompilerParams(collective_id=0, has_side_effects=True, vmem_limit_bytes=54500 * 1024),
    )(queries, keys, values)


def solution(mesh):
    outer, inner = mesh.shape["outer"], mesh.shape["inner"]

    def body(queries, keys, values):
        heads = queries.shape[2] // HEAD_DIM
        if outer % (2 * COLUMNS) == 0 and heads % outer == 0:
            return per_device(outer, inner, queries, keys, values)
        return per_device_split(queries, keys, values)

    return jax.shard_map(
        body,
        mesh=mesh,
        in_specs=(P("outer", None, "inner"),) * 3,
        out_specs=P(("outer", "inner"), None, None),
        check_vma=False,
    )
```
